32 devices in a mesh: freq: 4 (over y, x), row: 8 (over z, core).
Axes of the slice: x: 2, y: 2, z: 4, core: 2. Of those that a mesh axis runs over, the one named last changes fastest.
Arguments:
- data: bfloat16 [4, 2, 2048, 2048], P('freq', None, 'row'), may hold values from -60 to 60
Outputs:
- solution: float32 [4, 2, 2048, 2048], P('freq', None, 'row')
- direction: float32 [4, 2, 2048, 2048], P('freq', None, 'row')
The draws below stay inside these ranges and needn't reach their ends.
All inputs are finite; a program needn't handle non-finite values.
Results may differ from the reference program's by a relative error of at most 0.0042.
Values may be sent and summed in bfloat16 or wider, within the bound.
A program may use at most 128 MiB of HBM per device.

```python
import math
import jax
import jax.numpy as jnp
from jax import lax

STATIONS = 2048
ITERS = 2
FREQS = 4


def draw_data(key, part):
    keys = jax.random.split(jax.random.fold_in(key, 11), 3)
    noise = jnp.clip(jax.random.normal(keys[0], (FREQS, 2, STATIONS, STATIONS), jnp.float32), -4.0, 4.0)
    rise_rows = 3.0 ** (jnp.arange(STATIONS, dtype=jnp.float32) / max(STATIONS - 1, 1) - 1.0)
    rise_freq = 3.0 ** (jnp.arange(FREQS, dtype=jnp.float32) / max(FREQS - 1, 1) - 1.0)
    jitter = jnp.exp(jax.random.uniform(keys[1], (FREQS, 1, STATIONS, 1), jnp.float32, math.log(0.7), math.log(1.4)))
    columns = jnp.exp(jax.random.uniform(keys[2], (FREQS, 1, 1, STATIONS), jnp.float32, math.log(0.5), math.log(2.0)))
    scaled = noise * jitter * columns * rise_rows[None, None, :, None] * rise_freq[:, None, None, None]
    return scaled.astype(jnp.bfloat16)


def setup_inputs(seed: int = 0) -> dict:
    key_list = jax.random.split(jax.random.key(seed), 2)
    data = draw_data(jax.random.fold_in(key_list[1], 71), 0)
    return dict(data=data)


def coupling():
    return 1.0 / (3.0 * (2.0 * STATIONS) ** 0.5)

def rounded_copy(field):
    rounded = lax.optimization_barrier(field.astype(jnp.bfloat16))
    return rounded.astype(jnp.float32)

def forward_map(field, data):
    rounded = rounded_copy(field)
    slices = data.astype(jnp.float32)
    best = lax.Precision.HIGHEST
    real_part = jnp.einsum('frk,fkn->frn', rounded[:, 0], slices[:, 0], precision=best) - jnp.einsum('frk,fkn->frn', rounded[:, 1], slices[:, 1], precision=best)
    imag_part = jnp.einsum('frk,fkn->frn', rounded[:, 0], slices[:, 1], precision=best) + jnp.einsum('frk,fkn->frn', rounded[:, 1], slices[:, 0], precision=best)
    return field - coupling() * jnp.stack([real_part, imag_part], axis=1)

def adjoint_map(field, data):
    rounded = rounded_copy(field)
    slices = data.astype(jnp.float32)
    best = lax.Precision.HIGHEST
    real_part = jnp.einsum('frk,fnk->frn', rounded[:, 0], slices[:, 0], precision=best) + jnp.einsum('frk,fnk->frn', rounded[:, 1], slices[:, 1], precision=best)
    imag_part = jnp.einsum('frk,fnk->frn', rounded[:, 1], slices[:, 0], precision=best) - jnp.einsum('frk,fnk->frn', rounded[:, 0], slices[:, 1], precision=best)
    return field - coupling() * jnp.stack([real_part, imag_part], axis=1)

def pair_step(data_raw, model_unit, data):
    beta_now = jnp.sqrt(jnp.sum(data_raw * data_raw))
    image = adjoint_map(data_raw, data)
    model_raw = image / beta_now - beta_now * model_unit
    alpha_now = jnp.sqrt(jnp.sum(model_raw * model_raw))
    return (beta_now, data_raw / beta_now, model_raw, alpha_now, model_raw / alpha_now)

def reference(data):
    observed = data.astype(jnp.float32)
    zeros = jnp.zeros_like(observed)
    beta_now, data_unit, model_raw, alpha_now, model_unit = pair_step(observed, zeros, data)
    solution = zeros
    direction = model_unit
    phi_bar = beta_now
    rho_bar = alpha_now
    for iteration in range(ITERS):
        data_raw = forward_map(model_raw, data) / alpha_now - alpha_now * data_unit
        beta_now, data_unit, model_raw, alpha_now, model_unit = pair_step(data_raw, model_unit, data)
        rho_value = jnp.sqrt(rho_bar * rho_bar + beta_now * beta_now)
        cosine = rho_bar / rho_value
        sine_value = beta_now / rho_value
        theta_value = sine_value * alpha_now
        rho_bar = -cosine * alpha_now
        phi_value = cosine * phi_bar
        phi_bar = sine_value * phi_bar
        solution = solution + phi_value / rho_value * direction
        direction = model_unit - theta_value / rho_value * direction
    return (solution, direction)
```

```python
import functools

import jax
import jax.numpy as jnp
from jax import lax
from jax.experimental import pallas as pl
from jax.experimental.pallas import tpu as pltpu
from jax.sharding import PartitionSpec as P

ITERS = 2
MESH = pl.DeviceIdType.MESH
F32 = jnp.float32
BF16 = jnp.bfloat16


def dot(a, b):
    return lax.dot_general(a, b, (((1,), (0,)), ((), ())), preferred_element_type=F32)


def dot_t(a, b):
    return lax.dot_general(a, b, (((1,), (1,)), ((), ())), preferred_element_type=F32)


def lane_sums(x):
    s = jnp.sum(x, axis=0, keepdims=True)
    return functools.reduce(jnp.add, [s[:, i : i + 128] for i in range(0, s.shape[1], 128)])


def kernel(
    n, nf, weight, data, *refs,
):
    models, image, coef, refs = refs[:ITERS], refs[ITERS], refs[ITERS + 1], refs[ITERS + 2 :]
    (
        full, va, vd, d_raw, work, stats, slots, sums, fslots,
        load_sem, ssem, rsem, st_s, st_r, sf_s, sf_r,
    ) = refs
    m_raw = models[0]
    rows, order = data.shape[2], data.shape[3]
    m = n // 2
    me = lax.axis_index("row")
    mf = lax.axis_index("freq")
    z, c = lax.div(me, 2), lax.rem(me, 2)
    overlap = rows % 128 == 0
    unit = rows if overlap else min(order, 256)
    wide = min(order // 2, 512)

    def at_row(r):
        return {"row": r}

    def halves(body, between):
        count = order // wide
        pl.loop(0, count // 2)(body)
        between()
        pl.loop(count // 2, count)(body)

    def piece(zb, cc, p):
        start = pl.multiple_of((zb * 2 + cc) * rows, rows)
        return full.at[p, pl.ds(start, rows), :]

    loads = []
    for p in range(2):
        loads.append(pltpu.make_async_copy(data.at[0, p], piece(z, c, p), load_sem.at[p]))
        loads.append(
            pltpu.make_async_copy(
                data.at[0, p], vd.at[pl.ds(p * rows, rows), :], load_sem.at[2 + p]
            )
        )
    for copy in loads:
        copy.start()

    barrier = pltpu.get_barrier_semaphore()

    @pl.loop(1, n)
    def _(k):
        pl.semaphore_signal(
            barrier, inc=1, device_id=at_row(lax.rem(me + k, n)), device_id_type=MESH
        )

    @pl.loop(1, nf)
    def _(k):
        pl.semaphore_signal(
            barrier, inc=1, device_id={"freq": lax.rem(mf + k, nf)}, device_id_type=MESH
        )

    for copy in loads:
        copy.wait()

    stats[...] = jnp.zeros_like(stats)
    pl.semaphore_wait(barrier, n - 1 + nf - 1)

    def row_stat(k, j):
        return pltpu.make_async_remote_copy(
            src_ref=stats.at[k], dst_ref=slots.at[k, me], send_sem=st_s.at[k, j],
            recv_sem=st_r.at[k, me], device_id=at_row(j), device_id_type=MESH,
        )

    def row_arrival(k, j):
        return pltpu.make_async_remote_copy(
            src_ref=stats.at[k], dst_ref=slots.at[k, j], send_sem=st_s.at[k, j],
            recv_sem=st_r.at[k, j], device_id=at_row(j), device_id_type=MESH,
        )

    def freq_stat(k, j):
        return pltpu.make_async_remote_copy(
            src_ref=sums.at[k], dst_ref=fslots.at[k, mf], send_sem=sf_s.at[k, j],
            recv_sem=sf_r.at[k, mf], device_id={"freq": j}, device_id_type=MESH,
        )

    def freq_arrival(k, j):
        return pltpu.make_async_remote_copy(
            src_ref=sums.at[k], dst_ref=fslots.at[k, j], send_sem=sf_s.at[k, j],
            recv_sem=sf_r.at[k, j], device_id={"freq": j}, device_id_type=MESH,
        )

    def start_sum(k):
        slots[k, me] = stats[k]

        @pl.loop(1, n)
        def _(i):
            row_stat(k, lax.rem(me + i, n)).start()

    def middle_sum(k):
        @pl.loop(1, n)
        def _(i):
            row_arrival(k, lax.rem(me + i, n)).wait_recv()

        total = lax.fori_loop(
            1, n, lambda j, t: t + slots[k, j], slots[k, 0]
        )
        sums[k] = total
        fslots[k, mf] = total

        @pl.loop(1, nf)
        def _(i):
            freq_stat(k, lax.rem(mf + i, nf)).start()

    def finish_sum(k):
        @pl.loop(1, nf)
        def _(i):
            freq_arrival(k, lax.rem(mf + i, nf)).wait_recv()

        total = lax.fori_loop(
            1, nf, lambda j, t: t + fslots[k, j], fslots[k, 0]
        )
        values = jnp.sum(total, axis=1, keepdims=True)
        return [values[q : q + 1, :] for q in range(4)]

    def drain_sum(k):
        @pl.loop(1, n)
        def _(i):
            row_stat(k, lax.rem(me + i, n)).wait_send()

        @pl.loop(1, nf)
        def _(i):
            freq_stat(k, lax.rem(mf + i, nf)).wait_send()

    def block_copy(lane, zb, cc, p, target):
        return pltpu.make_async_remote_copy(
            src_ref=piece(zb, cc, p), dst_ref=piece(zb, cc, p),
            send_sem=ssem.at[lane, zb, p], recv_sem=rsem.at[zb * 2 + cc, p],
            device_id=at_row(target), device_id_type=MESH,
        )

    sibling = z * 2 + (1 - c)

    def spread(zb, p, below, above):
        @pl.when(below & (z + 1 < m))
        def _():
            block_copy(0, zb, c, p, lax.rem(me + 2, n)).start()

        @pl.when(above & (z > 0))
        def _():
            block_copy(1, zb, c, p, lax.rem(me + n - 2, n)).start()

        block_copy(2, zb, c, p, sibling).start()

    def settle(zb, p):
        @pl.when((zb <= z) & (z + 1 < m))
        def _():
            block_copy(0, zb, c, p, lax.rem(me + 2, n)).wait_send()

        @pl.when((zb >= z) & (z > 0))
        def _():
            block_copy(1, zb, c, p, lax.rem(me + n - 2, n)).wait_send()

        block_copy(2, zb, c, p, sibling).wait_send()

    spread(z, 0, jnp.bool_(True), jnp.bool_(True))

    @pl.loop(0, order // wide)
    def _(i):
        x = vd[:, pl.ds(pl.multiple_of(i * wide, wide), wide)].astype(F32)
        stats[0, 0:1, :] += lane_sums(x * x)

    start_sum(0)
    spread(z, 1, jnp.bool_(True), jnp.bool_(True))

    @pl.loop(0, order // wide)
    def _(i):
        cols = pl.ds(pl.multiple_of(i * wide, wide), wide)
        work[:, cols] = jnp.zeros((2 * rows, wide), F32)

    middle_sum(0)
    beta = jnp.sqrt(finish_sum(0)[0])

    def process(start):
        band = pl.ds(pl.multiple_of(start, unit), unit)
        tr = dot_t(vd[...], full[0, band, :])
        ti = dot_t(vd[...], full[1, band, :])
        fit = jnp.concatenate([tr[:rows] + ti[rows:], tr[rows:] - ti[:rows]], axis=0)
        raw = (vd[:, band].astype(F32) - weight * fit) / beta
        m_raw[:, band] = raw
        stats[1, 0:1, :] += lane_sums(raw * raw)
        va[:, band] = raw.astype(BF16)

        @pl.loop(0, order // wide)
        def _(i):
            cols = pl.ds(pl.multiple_of(i * wide, wide), wide)
            v = va[:, band]
            a = dot(v, full[0, band, cols])
            b = dot(v, full[1, band, cols])
            work[:, cols] += jnp.concatenate(
                [a[:rows] - b[rows:], a[rows:] + b[:rows]], axis=0
            )

    @pl.loop(0, m)
    def _(s):
        @pl.when(s > 0)
        def _():
            for p in range(2):
                @pl.when(z - s >= 0)
                def _():
                    block_copy(0, z - s, c, p, sibling).wait_recv()
                    spread(z - s, p, jnp.bool_(True), jnp.bool_(False))

                @pl.when(z + s < m)
                def _():
                    block_copy(0, z + s, c, p, sibling).wait_recv()
                    spread(z + s, p, jnp.bool_(False), jnp.bool_(True))

        @pl.loop(0, 4)
        def _(t):
            up = lax.div(t, 2)
            other = lax.rem(t, 2)
            zb = z - s + 2 * s * up
            cc = c + other * (1 - 2 * c)

            @pl.when((zb >= 0) & (zb < m) & ((s > 0) | (t < 2)))
            def _():
                @pl.when(other == 1)
                def _():
                    for p in range(2):
                        block_copy(0, zb, cc, p, sibling).wait_recv()

                if overlap:
                    process((zb * 2 + cc) * rows)

    if not overlap:
        @pl.loop(0, order // unit)
        def _(u):
            process(u * unit)

    start_sum(1)
    middle_sum(1)
    alpha = jnp.sqrt(finish_sum(1)[0])

    phi_bar, rho_bar = beta, alpha
    direction, answer = [1.0 / alpha], []
    for it in range(ITERS):
        last = it == ITERS - 1
        model_ref = models[it]
        ka, kb = 2 * it + 1, 2 * it + 2

        if it > 0:
            def forward(i):
                cols = pl.ds(pl.multiple_of(i * wide, wide), wide)
                a = dot(va[...], full[0, :, cols])
                b = dot(va[...], full[1, :, cols])
                work[:, cols] = jnp.concatenate(
                    [a[:rows] - b[rows:], a[rows:] + b[:rows]], axis=0
                )

            halves(forward, lambda: middle_sum(ka))
            alpha = jnp.sqrt(finish_sum(ka)[0])
            rotate(alpha)
        inv_alpha, keep = 1.0 / alpha, alpha / beta

        @pl.loop(0, order // wide)
        def _(i):
            cols = pl.ds(pl.multiple_of(i * wide, wide), wide)
            old = vd[:, cols].astype(F32) if it == 0 else d_raw[:, cols]
            new = (model_ref[:, cols] - weight * work[:, cols]) * inv_alpha - keep * old
            d_raw[:, cols] = new
            vd[:, cols] = new.astype(BF16)
            stats[kb, 0:1, :] += lane_sums(new * new)

        start_sum(kb)

        def adjoint(i):
            cols = pl.ds(pl.multiple_of(i * wide, wide), wide)
            tr = dot_t(vd[...], full[0, cols, :])
            ti = dot_t(vd[...], full[1, cols, :])
            fit = jnp.concatenate([tr[:rows] + ti[rows:], tr[rows:] - ti[:rows]], axis=0)
            new = d_raw[:, cols] - weight * fit
            image[:, cols] = new
            if last:
                stats[kb + 1, 0:1, :] += lane_sums(new * new)
                stats[kb + 1, 1:2, :] += lane_sums(new * model_ref[:, cols])

        halves(adjoint, lambda: middle_sum(kb))
        if last:
            start_sum(kb + 1)
        data_sq = finish_sum(kb)[0]
        beta = jnp.sqrt(data_sq)
        inv_beta, shift = 1.0 / beta, beta / alpha

        if not last:
            @pl.loop(0, order // wide)
            def _(i):
                cols = pl.ds(pl.multiple_of(i * wide, wide), wide)
                new = image[:, cols] * inv_beta - shift * model_ref[:, cols]
                models[it + 1][:, cols] = new
                va[:, cols] = new.astype(BF16)
                stats[kb + 1, 0:1, :] += lane_sums(new * new)

            start_sum(kb + 1)

        rho = jnp.sqrt(rho_bar * rho_bar + beta * beta)
        cosine, sine = rho_bar / rho, beta / rho
        step = cosine * phi_bar / rho
        phi_bar = sine * phi_bar
        answer = [x + step * w for x, w in zip(answer + [0.0], direction)]

        def rotate(alpha, sine=sine, cosine=cosine, rho=rho):
            nonlocal rho_bar, direction
            rho_bar = -cosine * alpha
            turn = sine * alpha / rho
            direction = [-turn * w for w in direction] + [1.0 / alpha]

    middle_sum(kb + 1)
    image_sq, cross = finish_sum(kb + 1)[:2]
    new_alpha = jnp.sqrt(image_sq / data_sq - 2.0 * cross / alpha + data_sq)
    rotate(new_alpha)
    tip = direction.pop()
    direction[-1] = direction[-1] - tip * shift
    direction.append(tip * inv_beta)
    for q, value in enumerate(answer + direction):
        coef[q : q + 1, :] = jnp.broadcast_to(value, (1, 128))

    for k in range(2 + 2 * ITERS):
        drain_sum(k)

    @pl.loop(0, m)
    def _(zb):
        for p in range(2):
            settle(zb, p)


def combine(coef, *refs):
    basis, refs = refs[: ITERS + 1], refs[ITERS + 1 :]
    answer, direction, staged, sem = refs
    rows, order = answer.shape[2], answer.shape[3]
    high = min(rows, 64)
    per = rows // high

    def leave(t):
        out = (answer, direction)[t[0]]
        return pltpu.make_async_copy(
            staged.at[t[0], pl.ds(t[1] * rows + t[2] * high, high), :],
            out.at[0, t[1], pl.ds(t[2] * high, high), :],
            sem.at[t],
        )

    factors = [coef[q : q + 1, 0:1] for q in range(2 * ITERS + 1)]
    tiles = [(o, p, i) for p in range(2) for i in range(per) for o in range(2)]
    for p in range(2):
        for i in range(per):
            band = pl.ds(p * rows + i * high, high)
            parts = [b[band, :] for b in basis]
            for o in range(2):
                used = parts[: ITERS + o]
                staged[o, band, :] = sum(
                    factors[o * ITERS + k] * x for k, x in enumerate(used)
                )
                leave((o, p, i)).start()
    for t in tiles:
        leave(t).wait()


def on_device(n, nf, data):
    rows, order = data.shape[2], data.shape[3]
    weight = 1.0 / (3.0 * (2.0 * order) ** 0.5)
    field = pltpu.VMEM((2 * rows, order), F32)
    rounded = pltpu.VMEM((2 * rows, order), BF16)
    rounds = 2 + 2 * ITERS
    dma = pltpu.SemaphoreType.DMA
    vmem = pl.BlockSpec(memory_space=pltpu.VMEM)
    anywhere = pl.BlockSpec(memory_space=pl.ANY)
    *basis, coef = pl.pallas_call(
        functools.partial(kernel, n, nf, weight),
        out_shape=(field,) * (ITERS + 1) + (pltpu.VMEM((8, 128), F32),),
        in_specs=[anywhere],
        out_specs=(vmem,) * (ITERS + 2),
        scratch_shapes=[
            pltpu.VMEM((2, order, order), BF16),
            rounded, rounded, field, field,
            pltpu.VMEM((rounds, 8, 128), F32),
            pltpu.VMEM((rounds, n, 8, 128), F32),
            pltpu.VMEM((rounds, 8, 128), F32),
            pltpu.VMEM((rounds, nf, 8, 128), F32),
            dma((4,)), dma((3, n // 2, 2)), dma((n, 2)),
            dma((rounds, n)), dma((rounds, n)),
            dma((rounds, nf)), dma((rounds, nf)),
        ],
        compiler_params=pltpu.CompilerParams(
            collective_id=0, has_side_effects=True, vmem_limit_bytes=46 * 2**20
        ),
    )(data)
    out = jax.ShapeDtypeStruct(data.shape, F32)
    high = min(rows, 64)
    return pl.pallas_call(
        combine,
        out_shape=(out, out),
        in_specs=[vmem] * (ITERS + 2),
        out_specs=(anywhere, anywhere),
        scratch_shapes=[pltpu.VMEM((2, 2 * rows, order), F32), dma((2, 2, rows // high))],
        compiler_params=pltpu.CompilerParams(vmem_limit_bytes=24 * 2**20),
    )(coef, *basis)


def solution(mesh):
    spec = P("freq", None, "row", None)
    return jax.shard_map(
        functools.partial(on_device, mesh.shape["row"], mesh.shape["freq"]),
        mesh=mesh,
        in_specs=(spec,),
        out_specs=(spec, spec),
        check_vma=False,
    )
```

```python
import functools

import jax
import jax.numpy as jnp
from jax import lax
from jax.experimental import pallas as pl
from jax.experimental.pallas import tpu as pltpu
from jax.sharding import PartitionSpec as P

ITERS = 2
MESH = pl.DeviceIdType.MESH
F32 = jnp.float32
BF16 = jnp.bfloat16


def dot(a, b):
    return lax.dot_general(a, b, (((1,), (0,)), ((), ())), preferred_element_type=F32)


def dot_t(a, b):
    return lax.dot_general(a, b, (((1,), (1,)), ((), ())), preferred_element_type=F32)


def lane_sums(x):
    s = jnp.sum(x, axis=0, keepdims=True)
    return functools.reduce(jnp.add, [s[:, i : i + 128] for i in range(0, s.shape[1], 128)])


def kernel(
    n, nf, weight, data, *refs,
):
    models, image, coef, refs = refs[:ITERS], refs[ITERS], refs[ITERS + 1], refs[ITERS + 2 :]
    (
        full, va, vd, d_raw, work, stats, slots, sums, fslots,
        spot, seats, load_sem, ssem, rsem, st_s, st_r, sf_s, sf_r, cast_s, cast_r,
    ) = refs
    m_raw = models[0]
    rows, order = data.shape[2], data.shape[3]
    m = n // 2
    me = lax.axis_index("row")
    mf = lax.axis_index("freq")
    z, c = lax.div(me, 2), lax.rem(me, 2)
    overlap = rows % 128 == 0
    unit = rows if overlap else min(order, 256)
    wide = min(order // 2, 512)
    shadow = overlap and m >= 4
    voters = range(2, n - 2) if shadow else range(n)

    def at_row(r):
        return {"row": r}

    def halves(body, between):
        count = order // wide
        pl.loop(0, count // 2)(body)
        between()
        pl.loop(count // 2, count)(body)

    def piece(zb, cc, p):
        start = pl.multiple_of((zb * 2 + cc) * rows, rows)
        return full.at[p, pl.ds(start, rows), :]

    loads = []
    for p in range(2):
        loads.append(pltpu.make_async_copy(data.at[0, p], piece(z, c, p), load_sem.at[p]))
        loads.append(
            pltpu.make_async_copy(
                data.at[0, p], vd.at[pl.ds(p * rows, rows), :], load_sem.at[2 + p]
            )
        )
    for copy in loads:
        copy.start()

    barrier = pltpu.get_barrier_semaphore()

    @pl.loop(1, n)
    def _(k):
        pl.semaphore_signal(
            barrier, inc=1, device_id=at_row(lax.rem(me + k, n)), device_id_type=MESH
        )

    @pl.loop(1, nf)
    def _(k):
        pl.semaphore_signal(
            barrier, inc=1, device_id={"freq": lax.rem(mf + k, nf)}, device_id_type=MESH
        )

    for copy in loads:
        copy.wait()

    stats[...] = jnp.zeros_like(stats)
    pl.semaphore_wait(barrier, n - 1 + nf - 1)

    def row_stat(k, j):
        return pltpu.make_async_remote_copy(
            src_ref=stats.at[k], dst_ref=slots.at[k, me], send_sem=st_s.at[k, j],
            recv_sem=st_r.at[k, me], device_id=at_row(j), device_id_type=MESH,
        )

    def row_arrival(k, j):
        return pltpu.make_async_remote_copy(
            src_ref=stats.at[k], dst_ref=slots.at[k, j], send_sem=st_s.at[k, j],
            recv_sem=st_r.at[k, j], device_id=at_row(j), device_id_type=MESH,
        )

    def freq_stat(k, j):
        return pltpu.make_async_remote_copy(
            src_ref=sums.at[k], dst_ref=fslots.at[k, mf], send_sem=sf_s.at[k, j],
            recv_sem=sf_r.at[k, mf], device_id={"freq": j}, device_id_type=MESH,
        )

    def freq_arrival(k, j):
        return pltpu.make_async_remote_copy(
            src_ref=sums.at[k], dst_ref=fslots.at[k, j], send_sem=sf_s.at[k, j],
            recv_sem=sf_r.at[k, j], device_id={"freq": j}, device_id_type=MESH,
        )

    def start_sum(k):
        slots[k, me] = stats[k]

        @pl.loop(1, n)
        def _(i):
            row_stat(k, lax.rem(me + i, n)).start()

    def middle_sum(k):
        @pl.loop(1, n)
        def _(i):
            row_arrival(k, lax.rem(me + i, n)).wait_recv()

        total = lax.fori_loop(
            1, n, lambda j, t: t + slots[k, j], slots[k, 0]
        )
        sums[k] = total
        fslots[k, mf] = total

        @pl.loop(1, nf)
        def _(i):
            freq_stat(k, lax.rem(mf + i, nf)).start()

    def finish_sum(k):
        @pl.loop(1, nf)
        def _(i):
            freq_arrival(k, lax.rem(mf + i, nf)).wait_recv()

        total = lax.fori_loop(
            1, nf, lambda j, t: t + fslots[k, j], fslots[k, 0]
        )
        values = jnp.sum(total, axis=1, keepdims=True)
        return [values[q : q + 1, :] for q in range(4)]

    def drain_sum(k):
        @pl.loop(1, n)
        def _(i):
            row_stat(k, lax.rem(me + i, n)).wait_send()

        @pl.loop(1, nf)
        def _(i):
            freq_stat(k, lax.rem(mf + i, nf)).wait_send()

    def cast(k, j, g):
        return pltpu.make_async_remote_copy(
            src_ref=spot.at[k], dst_ref=seats.at[k, me * nf + mf],
            send_sem=cast_s.at[k, j, g], recv_sem=cast_r.at[k, me, mf],
            device_id={"row": j, "freq": g}, device_id_type=MESH,
        )

    def cast_arrival(k, j, g):
        return pltpu.make_async_remote_copy(
            src_ref=spot.at[k], dst_ref=seats.at[k, j * nf + g],
            send_sem=cast_s.at[k, j, g], recv_sem=cast_r.at[k, j, g],
            device_id={"row": j, "freq": g}, device_id_type=MESH,
        )

    def others(body):
        @pl.loop(1, n * nf)
        def _(i):
            to = lax.rem(me * nf + mf + i, n * nf)
            body(lax.div(to, nf), lax.rem(to, nf))

    def start_cast(k, row):
        values = jnp.sum(stats[row], axis=1, keepdims=True)
        lane = lax.broadcasted_iota(jnp.int32, (1, 128), 1)
        spot[k] = jnp.where(lane < 64, values[0:1], values[1:2])
        seats[k, me * nf + mf] = spot[k]
        others(lambda j, g: cast(k, j, g).start())

    def finish_cast(k, rows_in):
        @pl.loop(rows_in[0], rows_in[-1] + 1)
        def _(j):
            @pl.loop(0, nf)
            def _(g):
                @pl.when((j != me) | (g != mf))
                def _():
                    cast_arrival(k, j, g).wait_recv()

        total = lax.fori_loop(
            rows_in[0] * nf, (rows_in[-1] + 1) * nf,
            lambda j, t: t + seats[k, j], jnp.zeros((1, 128), F32),
        )
        return total[:, 0:1], total[:, 64:65]

    def block_copy(lane, zb, cc, p, target):
        return pltpu.make_async_remote_copy(
            src_ref=piece(zb, cc, p), dst_ref=piece(zb, cc, p),
            send_sem=ssem.at[lane, zb, p], recv_sem=rsem.at[zb * 2 + cc, p],
            device_id=at_row(target), device_id_type=MESH,
        )

    sibling = z * 2 + (1 - c)

    def spread(zb, p, below, above):
        @pl.when(below & (z + 1 < m))
        def _():
            block_copy(0, zb, c, p, lax.rem(me + 2, n)).start()

        @pl.when(above & (z > 0))
        def _():
            block_copy(1, zb, c, p, lax.rem(me + n - 2, n)).start()

        block_copy(2, zb, c, p, sibling).start()

    def settle(zb, p):
        @pl.when((zb <= z) & (z + 1 < m))
        def _():
            block_copy(0, zb, c, p, lax.rem(me + 2, n)).wait_send()

        @pl.when((zb >= z) & (z > 0))
        def _():
            block_copy(1, zb, c, p, lax.rem(me + n - 2, n)).wait_send()

        block_copy(2, zb, c, p, sibling).wait_send()

    spread(z, 0, jnp.bool_(True), jnp.bool_(True))

    @pl.loop(0, order // wide)
    def _(i):
        x = vd[:, pl.ds(pl.multiple_of(i * wide, wide), wide)].astype(F32)
        stats[0, 0:1, :] += lane_sums(x * x)

    start_sum(0)
    spread(z, 1, jnp.bool_(True), jnp.bool_(True))

    @pl.loop(0, order // wide)
    def _(i):
        cols = pl.ds(pl.multiple_of(i * wide, wide), wide)
        work[:, cols] = jnp.zeros((2 * rows, wide), F32)

    middle_sum(0)
    beta = jnp.sqrt(finish_sum(0)[0])

    def process(start):
        band = pl.ds(pl.multiple_of(start, unit), unit)
        tr = dot_t(vd[...], full[0, band, :])
        ti = dot_t(vd[...], full[1, band, :])
        fit = jnp.concatenate([tr[:rows] + ti[rows:], tr[rows:] - ti[:rows]], axis=0)
        raw = (vd[:, band].astype(F32) - weight * fit) / beta
        m_raw[:, band] = raw
        stats[1, 0:1, :] += lane_sums(raw * raw)
        va[:, band] = raw.astype(BF16)

        @pl.loop(0, order // wide)
        def _(i):
            cols = pl.ds(pl.multiple_of(i * wide, wide), wide)
            v = va[:, band]
            a = dot(v, full[0, band, cols])
            b = dot(v, full[1, band, cols])
            work[:, cols] += jnp.concatenate(
                [a[:rows] - b[rows:], a[rows:] + b[:rows]], axis=0
            )

    @pl.loop(0, m)
    def _(s):
        @pl.when(s > 0)
        def _():
            for p in range(2):
                @pl.when(z - s >= 0)
                def _():
                    block_copy(0, z - s, c, p, sibling).wait_recv()
                    spread(z - s, p, jnp.bool_(True), jnp.bool_(False))

                @pl.when(z + s < m)
                def _():
                    block_copy(0, z + s, c, p, sibling).wait_recv()
                    spread(z + s, p, jnp.bool_(False), jnp.bool_(True))

        @pl.loop(0, 4)
        def _(t):
            up = lax.div(t, 2)
            other = lax.rem(t, 2)
            zb = z - s + 2 * s * up
            cc = c + other * (1 - 2 * c)

            @pl.when((zb >= 0) & (zb < m) & ((s > 0) | (t < 2)))
            def _():
                @pl.when(other == 1)
                def _():
                    for p in range(2):
                        block_copy(0, zb, cc, p, sibling).wait_recv()

                if overlap:
                    process((zb * 2 + cc) * rows)

    if not overlap:
        @pl.loop(0, order // unit)
        def _(u):
            process(u * unit)

    if shadow:
        @pl.when((z == 1) | (z == m - 2))
        def _():
            edge = jnp.where(z == 1, 0, m - 1)
            vr, vi = piece(edge, c, 0), piece(edge, c, 1)

            @pl.loop(0, order // unit)
            def _(u):
                band = pl.ds(pl.multiple_of(u * unit, unit), unit)
                pr, pi = full.at[0, band, :], full.at[1, band, :]
                fr = dot_t(vr[...], pr[...]) + dot_t(vi[...], pi[...])
                raw = (vr[:, band].astype(F32) - weight * fr) / beta
                stats[1, 0:1, :] += lane_sums(raw * raw)
                fi = dot_t(vi[...], pr[...]) - dot_t(vr[...], pi[...])
                raw = (vi[:, band].astype(F32) - weight * fi) / beta
                stats[1, 0:1, :] += lane_sums(raw * raw)

    votes = (me >= voters[0]) & (me <= voters[-1])

    @pl.when(votes)
    def _():
        start_cast(0, 1)

    alpha = jnp.sqrt(finish_cast(0, voters)[0])

    phi_bar, rho_bar = beta, alpha
    direction, answer = [1.0 / alpha], []
    for it in range(ITERS):
        last = it == ITERS - 1
        model_ref = models[it]
        ka, kb = 2 * it + 1, 2 * it + 2

        if it > 0:
            def forward(i):
                cols = pl.ds(pl.multiple_of(i * wide, wide), wide)
                a = dot(va[...], full[0, :, cols])
                b = dot(va[...], full[1, :, cols])
                work[:, cols] = jnp.concatenate(
                    [a[:rows] - b[rows:], a[rows:] + b[:rows]], axis=0
                )

            halves(forward, lambda: middle_sum(ka))
            alpha = jnp.sqrt(finish_sum(ka)[0])
            rotate(alpha)
        inv_alpha, keep = 1.0 / alpha, alpha / beta

        @pl.loop(0, order // wide)
        def _(i):
            cols = pl.ds(pl.multiple_of(i * wide, wide), wide)
            old = vd[:, cols].astype(F32) if it == 0 else d_raw[:, cols]
            new = (model_ref[:, cols] - weight * work[:, cols]) * inv_alpha - keep * old
            d_raw[:, cols] = new
            vd[:, cols] = new.astype(BF16)
            stats[kb, 0:1, :] += lane_sums(new * new)

        start_sum(kb)

        def adjoint(i):
            cols = pl.ds(pl.multiple_of(i * wide, wide), wide)
            tr = dot_t(vd[...], full[0, cols, :])
            ti = dot_t(vd[...], full[1, cols, :])
            fit = jnp.concatenate([tr[:rows] + ti[rows:], tr[rows:] - ti[:rows]], axis=0)
            new = d_raw[:, cols] - weight * fit
            image[:, cols] = new
            if last:
                stats[kb + 1, 0:1, :] += lane_sums(new * new)
                stats[kb + 1, 1:2, :] += lane_sums(new * model_ref[:, cols])

        halves(adjoint, lambda: middle_sum(kb))
        if last:
            start_cast(1, kb + 1)
        data_sq = finish_sum(kb)[0]
        beta = jnp.sqrt(data_sq)
        inv_beta, shift = 1.0 / beta, beta / alpha

        if not last:
            @pl.loop(0, order // wide)
            def _(i):
                cols = pl.ds(pl.multiple_of(i * wide, wide), wide)
                new = image[:, cols] * inv_beta - shift * model_ref[:, cols]
                models[it + 1][:, cols] = new
                va[:, cols] = new.astype(BF16)
                stats[kb + 1, 0:1, :] += lane_sums(new * new)

            start_sum(kb + 1)

        rho = jnp.sqrt(rho_bar * rho_bar + beta * beta)
        cosine, sine = rho_bar / rho, beta / rho
        step = cosine * phi_bar / rho
        phi_bar = sine * phi_bar
        answer = [x + step * w for x, w in zip(answer + [0.0], direction)]

        def rotate(alpha, sine=sine, cosine=cosine, rho=rho):
            nonlocal rho_bar, direction
            rho_bar = -cosine * alpha
            turn = sine * alpha / rho
            direction = [-turn * w for w in direction] + [1.0 / alpha]

    @pl.loop(0, order // wide)
    def _(i):
        cols = pl.ds(pl.multiple_of(i * wide, wide), wide)
        parts = [model[:, cols] for model in models]
        models[0][:, cols] = sum(w * x for w, x in zip(answer, parts))
        models[1][:, cols] = sum(w * x for w, x in zip(direction, parts))
        image[:, cols] = inv_beta * image[:, cols] - shift * parts[-1]

    for k in (0, *range(2, 1 + 2 * ITERS)):
        drain_sum(k)

    @pl.loop(0, m)
    def _(zb):
        for p in range(2):
            settle(zb, p)

    @pl.when(votes)
    def _():
        others(lambda j, g: cast(0, j, g).wait_send())

    image_sq, cross = finish_cast(1, range(n))
    new_alpha = jnp.sqrt(image_sq / data_sq - 2.0 * cross / alpha + data_sq)
    coef[0:1, :] = jnp.broadcast_to(-sine * new_alpha / rho, (1, 128))
    coef[1:2, :] = jnp.broadcast_to(1.0 / new_alpha, (1, 128))
    others(lambda j, g: cast(1, j, g).wait_send())


def combine(coef, ready, turned, fresh, answer, direction, staged, sem):
    rows, order = answer.shape[2], answer.shape[3]
    high = min(rows, 64)
    per = rows // high

    def leave(o, p, i):
        source, out = ((ready, answer), (staged, direction))[o]
        return pltpu.make_async_copy(
            source.at[pl.ds(p * rows + i * high, high), :],
            out.at[0, p, pl.ds(i * high, high), :],
            sem.at[o, p, i],
        )

    tiles = [(p, i) for p in range(2) for i in range(per)]
    for p, i in tiles:
        leave(0, p, i).start()
    old, new = coef[0:1, 0:1], coef[1:2, 0:1]
    for p, i in tiles:
        band = pl.ds(p * rows + i * high, high)
        staged[band, :] = old * turned[band, :] + new * fresh[band, :]
        leave(1, p, i).start()
    for p, i in tiles:
        for o in range(2):
            leave(o, p, i).wait()


def on_device(n, nf, data):
    rows, order = data.shape[2], data.shape[3]
    weight = 1.0 / (3.0 * (2.0 * order) ** 0.5)
    field = pltpu.VMEM((2 * rows, order), F32)
    rounded = pltpu.VMEM((2 * rows, order), BF16)
    rounds = 2 + 2 * ITERS
    dma = pltpu.SemaphoreType.DMA
    vmem = pl.BlockSpec(memory_space=pltpu.VMEM)
    anywhere = pl.BlockSpec(memory_space=pl.ANY)
    *basis, coef = pl.pallas_call(
        functools.partial(kernel, n, nf, weight),
        out_shape=(field,) * (ITERS + 1) + (pltpu.VMEM((8, 128), F32),),
        in_specs=[anywhere],
        out_specs=(vmem,) * (ITERS + 2),
        scratch_shapes=[
            pltpu.VMEM((2, order, order), BF16),
            rounded, rounded, field, field,
            pltpu.VMEM((rounds, 8, 128), F32),
            pltpu.VMEM((rounds, n, 8, 128), F32),
            pltpu.VMEM((rounds, 8, 128), F32),
            pltpu.VMEM((rounds, nf, 8, 128), F32),
            pltpu.VMEM((2, 1, 128), F32), pltpu.VMEM((2, n * nf, 1, 128), F32),
            dma((4,)), dma((3, n // 2, 2)), dma((n, 2)),
            dma((rounds, n)), dma((rounds, n)),
            dma((rounds, nf)), dma((rounds, nf)),
            dma((2, n, nf)), dma((2, n, nf)),
        ],
        compiler_params=pltpu.CompilerParams(
            collective_id=0, has_side_effects=True, vmem_limit_bytes=46 * 2**20
        ),
    )(data)
    out = jax.ShapeDtypeStruct(data.shape, F32)
    high = min(rows, 64)
    return pl.pallas_call(
        combine,
        out_shape=(out, out),
        in_specs=[vmem] * (ITERS + 2),
        out_specs=(anywhere, anywhere),
        scratch_shapes=[pltpu.VMEM((2 * rows, order), F32), dma((2, 2, rows // high))],
        compiler_params=pltpu.CompilerParams(vmem_limit_bytes=24 * 2**20),
    )(coef, *basis)


def solution(mesh):
    spec = P("freq", None, "row", None)
    return jax.shard_map(
        functools.partial(on_device, mesh.shape["row"], mesh.shape["freq"]),
        mesh=mesh,
        in_specs=(spec,),
        out_specs=(spec, spec),
        check_vma=False,
    )
```

```python
import functools

import jax
import jax.numpy as jnp
from jax import lax
from jax.experimental import pallas as pl
from jax.experimental.pallas import tpu as pltpu
from jax.sharding import PartitionSpec as P

ITERS = 2
MESH = pl.DeviceIdType.MESH
F32 = jnp.float32
BF16 = jnp.bfloat16


def dot(a, b):
    return lax.dot_general(a, b, (((1,), (0,)), ((), ())), preferred_element_type=F32)


def dot_t(a, b):
    return lax.dot_general(a, b, (((1,), (1,)), ((), ())), preferred_element_type=F32)


def lane_sums(x):
    s = jnp.sum(x, axis=0, keepdims=True)
    return functools.reduce(jnp.add, [s[:, i : i + 128] for i in range(0, s.shape[1], 128)])


def block_sizes(rows, order):
    wide = min(order // 2, 512)
    return wide, 2 if rows % 256 == 0 and wide % (2 * rows) == 0 else 1


def kernel(
    n, nf, weight, data, *refs,
):
    models, image, coef, refs = refs[:ITERS], refs[ITERS], refs[ITERS + 1], refs[ITERS + 2 :]
    (
        full, va, vd, va_turned, vd_turned, d_raw, work, early, norms,
        stats, slots, sums, fslots, spot, seats,
        load_sem, ssem, rsem, sum_sem, cast_s, cast_r,
    ) = refs
    m_raw = models[0]
    rows, order = data.shape[2], data.shape[3]
    m = n // 2
    me = lax.axis_index("row")
    mf = lax.axis_index("freq")
    z, c = lax.div(me, 2), lax.rem(me, 2)
    sibling = z * 2 + (1 - c)
    wide, parts = block_sizes(rows, order)
    half = rows // parts
    count = order // wide
    overlap = rows % 128 == 0
    unit = 2 * half if overlap else min(order, 256)
    shadow = overlap and m >= 4
    edge = (z == 0) | (z == m - 1)
    voters = range(2, n - 2) if shadow else range(n)
    votes = (me >= voters[0]) & (me <= voters[-1])

    def at_row(r):
        return {"row": r}

    def wrap(x, size):
        return jnp.where(x >= size, x - size, x)

    def block(i):
        return pl.ds(pl.multiple_of(i * wide, wide), wide)

    def piece(zb, cc, h, p):
        start = pl.multiple_of(((zb * parts + h) * 2 + cc) * half, half)
        return full.at[p, pl.ds(start, half), :]

    def band_columns(u):
        if parts == 1:
            return [pl.ds(pl.multiple_of(u * unit, unit), unit)]
        base = lax.div(u, 2) * 2 * rows + lax.rem(u, 2) * half
        return [pl.ds(pl.multiple_of(base + cc * rows, half), half) for cc in range(2)]

    def regroup(x):
        if parts == 1:
            return x
        group = 2 * rows
        return jnp.concatenate(
            [
                x[:, g + k * half : g + (k + 1) * half]
                for g in range(0, x.shape[1], group)
                for k in (0, 2, 1, 3)
            ],
            axis=1,
        )

    loads = []
    for h in range(parts):
        for p in range(2):
            loads.append(
                pltpu.make_async_copy(
                    data.at[0, p, pl.ds(h * half, half), :],
                    piece(z, c, h, p), load_sem.at[h * 2 + p],
                )
            )
    for p in range(2):
        loads.append(
            pltpu.make_async_copy(
                data.at[0, p], vd.at[pl.ds(p * rows, rows), :], load_sem.at[2 * parts + p]
            )
        )
    for copy in loads:
        copy.start()

    barrier = pltpu.get_barrier_semaphore()

    @pl.loop(1, n)
    def _(k):
        pl.semaphore_signal(
            barrier, inc=1, device_id=at_row(wrap(me + k, n)), device_id_type=MESH
        )

    @pl.loop(1, nf)
    def _(k):
        pl.semaphore_signal(
            barrier, inc=1, device_id={"freq": wrap(mf + k, nf)}, device_id_type=MESH
        )

    stats[...] = jnp.zeros_like(stats)
    for copy in loads[: 2 * parts]:
        copy.wait()
    pl.semaphore_wait(barrier, n - 1 + nf - 1)

    def row_stat(j, seat):
        return pltpu.make_async_remote_copy(
            src_ref=stats.at[0], dst_ref=slots.at[seat], send_sem=sum_sem.at[0],
            recv_sem=sum_sem.at[1], device_id=at_row(j), device_id_type=MESH,
        )

    def freq_stat(j, seat):
        return pltpu.make_async_remote_copy(
            src_ref=sums, dst_ref=fslots.at[seat], send_sem=sum_sem.at[2],
            recv_sem=sum_sem.at[3], device_id={"freq": j}, device_id_type=MESH,
        )

    def bulk(ref, send_sem, recv_sem):
        return pltpu.make_async_remote_copy(
            src_ref=ref, dst_ref=ref, send_sem=send_sem, recv_sem=recv_sem,
            device_id=at_row(sibling), device_id_type=MESH,
        )

    def rows_bulk():
        return bulk(slots.at[pl.ds(0, n - 1)], sum_sem.at[0], sum_sem.at[1])

    def freqs_bulk():
        return bulk(fslots.at[pl.ds(0, nf - 1)], sum_sem.at[2], sum_sem.at[3])

    def start_sum():
        slots[me] = stats[0]

        @pl.loop(1, n)
        def _(i):
            row_stat(wrap(me + i, n), me).start()

    def finish_sum():
        rows_bulk().wait_recv()
        total = jnp.sum(slots[...], axis=0)
        sums[...] = total
        fslots[mf] = total

        @pl.loop(1, nf)
        def _(i):
            freq_stat(wrap(mf + i, nf), mf).start()

        freqs_bulk().wait_recv()
        return jnp.sum(jnp.sum(fslots[...], axis=0), axis=1, keepdims=True)[0:1]

    def drain_sum():
        rows_bulk().wait_send()
        freqs_bulk().wait_send()

    def cast(k, j, g):
        return pltpu.make_async_remote_copy(
            src_ref=spot.at[k], dst_ref=seats.at[k, me * nf + mf],
            send_sem=cast_s.at[k], recv_sem=cast_r.at[k],
            device_id={"row": j, "freq": g}, device_id_type=MESH,
        )

    def cast_bulk(k, number):
        return bulk(seats.at[k, pl.ds(0, number)], cast_s.at[k], cast_r.at[k])

    def others(body):
        @pl.loop(0, n)
        def _(i):
            j = wrap(me + i, n)
            for e in range(nf):
                if e:
                    body(j, wrap(mf + e, nf))
                else:
                    pl.when(i > 0)(lambda: body(j, mf))

    def start_cast(k):
        values = jnp.sum(stats[k + 1], axis=1, keepdims=True)
        lane = lax.broadcasted_iota(jnp.int32, (1, 128), 1)
        spot[k] = jnp.where(lane < 64, values[0:1], values[1:2])
        seats[k, me * nf + mf] = spot[k]
        others(lambda j, g: cast(k, j, g).start())

    def finish_cast(k, members):
        number = len(members) * nf
        if number == n * nf:
            cast_bulk(k, number - 1).wait_recv()
        else:
            pl.when(votes)(lambda: cast_bulk(k, number - 1).wait_recv())
            pl.when(jnp.logical_not(votes))(lambda: cast_bulk(k, number).wait_recv())

        held = seats[k, members[0] * nf : (members[-1] + 1) * nf]
        total = jnp.sum(held, axis=0)
        return total[:, 0:1], total[:, 64:65]

    def drain_cast(k):
        cast_bulk(k, n * nf - 1).wait_send()

    def block_copy(lane, zb, cc, h, p, target):
        return pltpu.make_async_remote_copy(
            src_ref=piece(zb, cc, h, p), dst_ref=piece(zb, cc, h, p),
            send_sem=ssem.at[lane], recv_sem=rsem.at[zb * 2 + cc, h, p],
            device_id=at_row(target), device_id_type=MESH,
        )

    above_me, below_me = wrap(me + 2, n), wrap(me + n - 2, n)

    def spread(zb, h, p, up, down):
        if up:
            @pl.when(z + 1 < m)
            def _():
                block_copy(0, zb, c, h, p, above_me).start()

        if down:
            @pl.when(z > 0)
            def _():
                block_copy(1, zb, c, h, p, below_me).start()

        block_copy(2, zb, c, h, p, sibling).start()

    def settle():
        def sent(lane, blocks):
            bulk(full.at[0, pl.ds(0, 2 * rows * blocks), :], ssem.at[lane], ssem.at[lane]).wait_send()

        for k in range(m):
            @pl.when(z == k)
            def _():
                if k < m - 1:
                    sent(0, k + 1)
                if k > 0:
                    sent(1, m - k)

        sent(2, m)

    def await_piece(zb, cc, h, p):
        block_copy(0, zb, cc, h, p, sibling).wait_recv()

    for p in range(2):
        spread(z, 0, p, True, True)
    for copy in loads[2 * parts :]:
        copy.wait()

    def keep_data(columns, x):
        vd[:, columns] = x
        vd_turned[:rows, columns] = x[rows:]
        vd_turned[rows:, columns] = -x[:rows]

    def keep_model(columns, x):
        va[:, columns] = x
        va_turned[:rows, columns] = -x[rows:]
        va_turned[rows:, columns] = x[:rows]

    @pl.loop(0, count)
    def _(i):
        x = vd[:, block(i)]
        vd_turned[:rows, block(i)] = x[rows:]
        vd_turned[rows:, block(i)] = -x[:rows]
        x = x.astype(F32)
        stats[0, 0:1, :] += lane_sums(x * x)

    start_sum()
    for h in range(1, parts):
        for p in range(2):
            spread(z, h, p, True, True)

    @pl.loop(0, count)
    def _(i):
        work[:, block(i)] = jnp.zeros((2 * rows, wide), F32)

    beta = jnp.sqrt(finish_sum())

    def forward_fit(low, columns):
        return dot(va[:, low], full[0, low, columns]) + dot(va_turned[:, low], full[1, low, columns])

    def adjoint_fit(band):
        return dot_t(vd[...], full[0, band, :]) + dot_t(vd_turned[...], full[1, band, :])

    def gather_columns(ref, slices):
        return jnp.concatenate([ref[:, s] for s in slices], axis=1)

    def begin(u):
        band = pl.ds(pl.multiple_of(u * unit, unit), unit)
        early[...] = dot_t(vd[...], full[0, band, :])

    def process(u, leave, split=False):
        band = pl.ds(pl.multiple_of(u * unit, unit), unit)
        slices = band_columns(u)
        fit = early[...] + dot_t(vd_turned[...], full[1, band, :]) if split else adjoint_fit(band)
        raw = (gather_columns(vd, slices).astype(F32) - weight * fit) / beta
        width = raw.shape[1] // len(slices)
        for k, columns in enumerate(slices):
            m_raw[:, columns] = raw[:, k * width : (k + 1) * width]
        stats[1, 0:1, :] += lane_sums(raw * raw)
        keep_model(band, raw.astype(BF16))

        def visit(i):
            leave(i, work[:, block(i)] + forward_fit(band, block(i)))

        if split:
            for i in range(count):
                visit(i)
        else:
            pl.loop(0, count)(visit)

    def keep_work(i, value):
        work[:, block(i)] = value

    def update_data(it, alpha, beta, i, fit):
        columns = block(i)
        old = vd[:, columns].astype(F32) if it == 0 else d_raw[:, columns]
        new = (models[it][:, columns] - weight * fit) * (1.0 / alpha) - (alpha / beta) * old
        d_raw[:, columns] = new
        keep_data(columns, new.astype(BF16))
        stats[2 * it + 2, 0:1, :] += lane_sums(new * new)

    @pl.loop(0, m - 1 if shadow else m)
    def _(s):
        for h in range(parts):
            @pl.when(s > 0)
            def _():
                for p in range(2):
                    @pl.when(z - s >= 0)
                    def _():
                        await_piece(z - s, c, h, p)
                        spread(z - s, h, p, True, False)

                    @pl.when(z + s < m)
                    def _():
                        await_piece(z + s, c, h, p)
                        spread(z + s, h, p, False, True)

            @pl.loop(0, 2)
            def _(up):
                zb = z - s + 2 * s * up

                @pl.when((zb >= 0) & (zb < m) & ((s > 0) | (up == 0)))
                def _():
                    for p in range(2):
                        await_piece(zb, 1 - c, h, p)
                    if overlap:
                        process(zb * parts + h, keep_work)

    if not overlap:
        @pl.loop(0, order // unit)
        def _(u):
            process(u, keep_work)

    def first_alpha():
        alpha = jnp.sqrt(finish_cast(0, voters)[0])
        norms[0:1, :] = jnp.broadcast_to(alpha, (1, 128))
        return alpha

    def update_all():
        alpha = first_alpha()

        @pl.loop(0, count)
        def _(i):
            update_data(0, alpha, beta, i, work[:, block(i)])

    if shadow:
        @pl.when(jnp.logical_not(edge))
        def _():
            @pl.when((z == 1) | (z == m - 2))
            def _():
                home = jnp.where(z == 1, 0, m - 1)
                if parts == 1:
                    mine = [(home * 2 + c) * rows]
                    high = rows
                else:
                    mine = [(home * parts + c) * unit]
                    high = unit
                mine = [pl.ds(pl.multiple_of(x, high), high) for x in mine]
                for low in mine:
                    @pl.loop(0, order // unit)
                    def _(u):
                        band = pl.ds(pl.multiple_of(u * unit, unit), unit)
                        slices = band_columns(u)
                        for p in range(2):
                            fit = dot_t(full[p, low, :], full[0, band, :])
                            other = dot_t(full[1 - p, low, :], full[1, band, :])
                            fit = fit - other if p else fit + other
                            x = jnp.concatenate([full[p, low, s] for s in slices], axis=1)
                            raw = (x.astype(F32) - weight * fit) / beta
                            stats[1, 0:1, :] += lane_sums(raw * raw)

            start_cast(0)
            update_all()

        @pl.when(edge)
        def _():
            zb = m - 1 - z
            for h in range(parts):
                u = zb * parts + h
                for p in range(2):
                    await_piece(zb, c, h, p)
                    block_copy(2, zb, c, h, p, sibling).start()
                    await_piece(zb, 1 - c, h, p)
                    if p == 0 and h == parts - 1:
                        begin(u)
                if h < parts - 1:
                    process(u, keep_work)
                else:
                    alpha = first_alpha()
                    process(u, functools.partial(update_data, 0, alpha, beta), True)
    else:
        start_cast(0)
        update_all()

    alpha = norms[0:1, 0:1]
    phi_bar, rho_bar = beta, alpha
    direction, answer = [1.0 / alpha], []
    everyone = range(n)
    lead = count - 1
    for it in range(ITERS):
        last = it == ITERS - 1
        ka, kb = 2 * it, 2 * it + 1
        model_ref = models[it]
        low = pl.ds(0, order)

        if it > 0:
            @pl.loop(0, lead)
            def _(i):
                work[:, block(i)] = forward_fit(low, block(i))

            alpha = jnp.sqrt(finish_cast(ka, everyone)[0])
            for i in range(lead, count):
                fit = forward_fit(low, block(i))
                for j in range(i * lead // count if i < count - 1 else 0, lead):
                    update_data(it, alpha, beta, j, work[:, block(j)])
                update_data(it, alpha, beta, i, fit)
            rotate(alpha)
        start_cast(kb)

        def adjoint_image(i):
            return d_raw[:, block(i)] - weight * regroup(adjoint_fit(block(i)))

        if last:
            @pl.loop(0, count)
            def _(i):
                new = adjoint_image(i)
                image[:, block(i)] = new
                stats[kb + 2, 0:1, :] += lane_sums(new * new)
                stats[kb + 2, 1:2, :] += lane_sums(new * model_ref[:, block(i)])

            start_cast(kb + 1)
        else:
            @pl.loop(0, lead)
            def _(i):
                image[:, block(i)] = adjoint_image(i)

        data_sq = finish_cast(kb, everyone)[0]
        beta = jnp.sqrt(data_sq)
        inv_beta, shift = 1.0 / beta, beta / alpha

        if not last:
            def update_model(i, value):
                new = value * inv_beta - shift * model_ref[:, block(i)]
                models[it + 1][:, block(i)] = new
                keep_model(block(i), regroup(new.astype(BF16)))
                stats[kb + 2, 0:1, :] += lane_sums(new * new)

            value = adjoint_image(lead)
            for j in range(lead):
                update_model(j, image[:, block(j)])
            update_model(lead, value)
            start_cast(kb + 1)

        rho = jnp.sqrt(rho_bar * rho_bar + beta * beta)
        cosine, sine = rho_bar / rho, beta / rho
        step = cosine * phi_bar / rho
        phi_bar = sine * phi_bar
        answer = [x + step * w for x, w in zip(answer + [0.0], direction)]

        def rotate(alpha, sine=sine, cosine=cosine, rho=rho):
            nonlocal rho_bar, direction
            rho_bar = -cosine * alpha
            turn = sine * alpha / rho
            direction = [-turn * w for w in direction] + [1.0 / alpha]

    @pl.loop(0, count)
    def _(i):
        basis = [model[:, block(i)] for model in models]
        models[0][:, block(i)] = sum(w * x for w, x in zip(answer, basis))
        models[1][:, block(i)] = sum(w * x for w, x in zip(direction, basis))
        image[:, block(i)] = inv_beta * image[:, block(i)] - shift * basis[-1]

    drain_sum()
    pl.when(votes)(lambda: drain_cast(0))
    for k in range(1, 2 * ITERS):
        drain_cast(k)

    settle()

    image_sq, cross = finish_cast(2 * ITERS, everyone)
    new_alpha = jnp.sqrt(image_sq / data_sq - 2.0 * cross / alpha + data_sq)
    coef[0:1, :] = jnp.broadcast_to(-sine * new_alpha / rho, (1, 128))
    coef[1:2, :] = jnp.broadcast_to(1.0 / new_alpha, (1, 128))
    drain_cast(2 * ITERS)


def combine(coef, ready, turned, fresh, answer, direction, staged, sem):
    rows, order = answer.shape[2], answer.shape[3]
    high = min(rows, 64)
    per = rows // high

    def leave(o, p, i):
        source, out = ((ready, answer), (staged, direction))[o]
        return pltpu.make_async_copy(
            source.at[pl.ds(p * rows + i * high, high), :],
            out.at[0, p, pl.ds(i * high, high), :],
            sem.at[o, p, i],
        )

    tiles = [(p, i) for p in range(2) for i in range(per)]
    for p, i in tiles:
        leave(0, p, i).start()
    old, new = coef[0:1, 0:1], coef[1:2, 0:1]
    for p, i in tiles:
        band = pl.ds(p * rows + i * high, high)
        staged[band, :] = old * turned[band, :] + new * fresh[band, :]
        leave(1, p, i).start()
    for p, i in tiles:
        for o in range(2):
            leave(o, p, i).wait()


def on_device(n, nf, data):
    rows, order = data.shape[2], data.shape[3]
    weight = 1.0 / (3.0 * (2.0 * order) ** 0.5)
    wide, parts = block_sizes(rows, order)
    unit = 2 * rows // parts if rows % 128 == 0 else min(order, 256)
    field = pltpu.VMEM((2 * rows, order), F32)
    rounded = pltpu.VMEM((2 * rows, order), BF16)
    tile = pltpu.VMEM((8, 128), F32)
    casts = 1 + 2 * ITERS
    dma = pltpu.SemaphoreType.DMA
    vmem = pl.BlockSpec(memory_space=pltpu.VMEM)
    anywhere = pl.BlockSpec(memory_space=pl.ANY)
    *basis, coef = pl.pallas_call(
        functools.partial(kernel, n, nf, weight),
        out_shape=(field,) * (ITERS + 1) + (tile,),
        in_specs=[anywhere],
        out_specs=(vmem,) * (ITERS + 2),
        scratch_shapes=[
            pltpu.VMEM((2, order, order), BF16),
            rounded, rounded, rounded, rounded, field, field,
            pltpu.VMEM((2 * rows, unit), F32), tile,
            pltpu.VMEM((casts + 1, 8, 128), F32),
            pltpu.VMEM((n, 8, 128), F32), tile, pltpu.VMEM((nf, 8, 128), F32),
            pltpu.VMEM((casts, 1, 128), F32), pltpu.VMEM((casts, n * nf, 1, 128), F32),
            dma((2 * parts + 2,)), dma((3,)), dma((n, parts, 2)),
            dma((4,)), dma((casts,)), dma((casts,)),
        ],
        compiler_params=pltpu.CompilerParams(
            collective_id=0, has_side_effects=True, vmem_limit_bytes=46 * 2**20
        ),
    )(data)
    out = jax.ShapeDtypeStruct(data.shape, F32)
    high = min(rows, 64)
    return pl.pallas_call(
        combine,
        out_shape=(out, out),
        in_specs=[vmem] * (ITERS + 2),
        out_specs=(anywhere, anywhere),
        scratch_shapes=[pltpu.VMEM((2 * rows, order), F32), dma((2, 2, rows // high))],
        compiler_params=pltpu.CompilerParams(vmem_limit_bytes=24 * 2**20),
    )(coef, *basis)


def solution(mesh):
    spec = P("freq", None, "row", None)
    return jax.shard_map(
        functools.partial(on_device, mesh.shape["row"], mesh.shape["freq"]),
        mesh=mesh,
        in_specs=(spec,),
        out_specs=(spec, spec),
        check_vma=False,
    )
```

```python
import functools

import jax
import jax.numpy as jnp
from jax import lax
from jax.experimental import pallas as pl
from jax.experimental.pallas import tpu as pltpu
from jax.sharding import PartitionSpec as P

ITERS = 2
MESH = pl.DeviceIdType.MESH
F32 = jnp.float32
BF16 = jnp.bfloat16


def dot(a, b):
    return lax.dot_general(a, b, (((1,), (0,)), ((), ())), preferred_element_type=F32)


def dot_t(a, b):
    return lax.dot_general(a, b, (((1,), (1,)), ((), ())), preferred_element_type=F32)


def fold(x):
    tiles = [
        x[r : r + 8, i : i + 128]
        for r in range(0, x.shape[0], 8)
        for i in range(0, x.shape[1], 128)
    ]
    while len(tiles) > 1:
        tiles = [sum(tiles[k : k + 2][1:], tiles[k]) for k in range(0, len(tiles), 2)]
    return tiles[0]


def block_sizes(rows, order):
    wide = min(order // 2, 512)
    return wide, 2 if rows % 256 == 0 and wide % (2 * rows) == 0 else 1


def kernel(
    n, nf, weight, data, *refs,
):
    models, image, coef, refs = refs[:ITERS], refs[ITERS], refs[ITERS + 1], refs[ITERS + 2 :]
    (
        full, va, vd, va_turned, vd_turned, d_raw, work, early,
        stats, slots, sums, fslots, spot, seats,
        load_sem, ssem, rsem, sum_sem, cast_s, cast_r,
    ) = refs
    m_raw = models[0]
    rows, order = data.shape[2], data.shape[3]
    m = n // 2
    me = lax.axis_index("row")
    mf = lax.axis_index("freq")
    z, c = lax.div(me, 2), lax.rem(me, 2)
    sibling = z * 2 + (1 - c)
    wide, parts = block_sizes(rows, order)
    half = rows // parts
    count = order // wide
    overlap = rows % 128 == 0
    unit = 2 * half if overlap else min(order, 256)
    shadow = overlap and m >= 4
    edge = (z == 0) | (z == m - 1)
    voters = range(2, n - 2) if shadow else range(n)
    votes = (me >= voters[0]) & (me <= voters[-1])

    def at_row(r):
        return {"row": r}

    def wrap(x, size):
        return jnp.where(x >= size, x - size, x)

    def block(i):
        return pl.ds(pl.multiple_of(i * wide, wide), wide)

    def piece(zb, cc, h, p):
        start = pl.multiple_of(((zb * parts + h) * 2 + cc) * half, half)
        return full.at[p, pl.ds(start, half), :]

    def band_columns(u):
        if parts == 1:
            return [pl.ds(pl.multiple_of(u * unit, unit), unit)]
        base = lax.div(u, 2) * 2 * rows + lax.rem(u, 2) * half
        return [pl.ds(pl.multiple_of(base + cc * rows, half), half) for cc in range(2)]

    def regroup(x):
        if parts == 1:
            return x
        group = 2 * rows
        return jnp.concatenate(
            [
                x[:, g + k * half : g + (k + 1) * half]
                for g in range(0, x.shape[1], group)
                for k in (0, 2, 1, 3)
            ],
            axis=1,
        )

    loads = []
    for h in range(parts):
        for p in range(2):
            loads.append(
                pltpu.make_async_copy(
                    data.at[0, p, pl.ds(h * half, half), :],
                    piece(z, c, h, p), load_sem.at[h * 2 + p],
                )
            )
    for p in range(2):
        loads.append(
            pltpu.make_async_copy(
                data.at[0, p], vd.at[pl.ds(p * rows, rows), :], load_sem.at[2 * parts + p]
            )
        )
    for copy in loads:
        copy.start()

    barrier = pltpu.get_barrier_semaphore()

    @pl.loop(1, n)
    def _(k):
        pl.semaphore_signal(
            barrier, inc=1, device_id=at_row(wrap(me + k, n)), device_id_type=MESH
        )

    @pl.loop(1, nf)
    def _(k):
        pl.semaphore_signal(
            barrier, inc=1, device_id={"freq": wrap(mf + k, nf)}, device_id_type=MESH
        )

    stats[...] = jnp.zeros_like(stats)
    for copy in loads[: 2 * parts]:
        copy.wait()
    pl.semaphore_wait(barrier, n - 1 + nf - 1)

    def row_stat(j, seat):
        return pltpu.make_async_remote_copy(
            src_ref=stats.at[0, 0], dst_ref=slots.at[seat], send_sem=sum_sem.at[0],
            recv_sem=sum_sem.at[1], device_id=at_row(j), device_id_type=MESH,
        )

    def freq_stat(j, seat):
        return pltpu.make_async_remote_copy(
            src_ref=sums, dst_ref=fslots.at[seat], send_sem=sum_sem.at[2],
            recv_sem=sum_sem.at[3], device_id={"freq": j}, device_id_type=MESH,
        )

    def bulk(ref, send_sem, recv_sem):
        return pltpu.make_async_remote_copy(
            src_ref=ref, dst_ref=ref, send_sem=send_sem, recv_sem=recv_sem,
            device_id=at_row(sibling), device_id_type=MESH,
        )

    def rows_bulk():
        return bulk(slots.at[pl.ds(0, n - 1)], sum_sem.at[0], sum_sem.at[1])

    def freqs_bulk():
        return bulk(fslots.at[pl.ds(0, nf - 1)], sum_sem.at[2], sum_sem.at[3])

    def start_sum():
        slots[me] = stats[0, 0]

        @pl.loop(1, n)
        def _(i):
            row_stat(wrap(me + i, n), me).start()

    def finish_sum():
        rows_bulk().wait_recv()
        total = jnp.sum(slots[...], axis=0)
        sums[...] = total
        fslots[mf] = total

        @pl.loop(1, nf)
        def _(i):
            freq_stat(wrap(mf + i, nf), mf).start()

        freqs_bulk().wait_recv()
        total = jnp.sum(jnp.sum(fslots[...], axis=0), axis=0, keepdims=True)
        return jnp.sum(total, axis=1, keepdims=True)

    def drain_sum():
        rows_bulk().wait_send()
        freqs_bulk().wait_send()

    def cast(k, j, g):
        return pltpu.make_async_remote_copy(
            src_ref=spot.at[k], dst_ref=seats.at[k, me * nf + mf],
            send_sem=cast_s.at[k], recv_sem=cast_r.at[k],
            device_id={"row": j, "freq": g}, device_id_type=MESH,
        )

    def cast_bulk(k, number):
        return bulk(seats.at[k, pl.ds(0, number)], cast_s.at[k], cast_r.at[k])

    def others(body):
        if n * nf <= 64:
            for i in range(n):
                for e in range(nf):
                    if i or e:
                        body(wrap(me + i, n), wrap(mf + e, nf))
            return

        @pl.loop(0, n)
        def _(i):
            j = wrap(me + i, n)
            pl.when(i > 0)(lambda: body(j, mf))
            for e in range(1, nf):
                body(j, wrap(mf + e, nf))

    def start_cast(k):
        first, second = [
            jnp.sum(jnp.sum(stats[k + 1, q], axis=0, keepdims=True), axis=1, keepdims=True)
            for q in range(2)
        ]
        lane = lax.broadcasted_iota(jnp.int32, (1, 128), 1)
        spot[k] = jnp.where(lane < 64, first, second)
        seats[k, me * nf + mf] = spot[k]
        others(lambda j, g: cast(k, j, g).start())

    def finish_cast(k, members):
        number = len(members) * nf
        if number == n * nf:
            cast_bulk(k, number - 1).wait_recv()
        else:
            pl.when(votes)(lambda: cast_bulk(k, number - 1).wait_recv())
            pl.when(jnp.logical_not(votes))(lambda: cast_bulk(k, number).wait_recv())

        held = seats[k, members[0] * nf : (members[-1] + 1) * nf]
        total = jnp.sum(held, axis=0)
        return total[:, 0:1], total[:, 64:65]

    def drain_cast(k):
        cast_bulk(k, n * nf - 1).wait_send()

    def block_copy(lane, zb, cc, h, p, target):
        return pltpu.make_async_remote_copy(
            src_ref=piece(zb, cc, h, p), dst_ref=piece(zb, cc, h, p),
            send_sem=ssem.at[lane], recv_sem=rsem.at[zb * 2 + cc, h, p],
            device_id=at_row(target), device_id_type=MESH,
        )

    above_me, below_me = wrap(me + 2, n), wrap(me + n - 2, n)

    def spread(zb, h, p, up, down):
        if up:
            @pl.when(z + 1 < m)
            def _():
                block_copy(0, zb, c, h, p, above_me).start()

        if down:
            @pl.when(z > 0)
            def _():
                block_copy(1, zb, c, h, p, below_me).start()

        block_copy(2, zb, c, h, p, sibling).start()

    def settle():
        def sent(lane, blocks):
            bulk(full.at[0, pl.ds(0, 2 * rows * blocks), :], ssem.at[lane], ssem.at[lane]).wait_send()

        for k in range(m):
            @pl.when(z == k)
            def _():
                if k < m - 1:
                    sent(0, k + 1)
                if k > 0:
                    sent(1, m - k)

        sent(2, m)

    def await_piece(zb, cc, h, p):
        block_copy(0, zb, cc, h, p, sibling).wait_recv()

    for p in range(2):
        spread(z, 0, p, True, True)
    for copy in loads[2 * parts :]:
        copy.wait()

    high = 64 if rows % 64 == 0 else 16

    def sweep(body, stat):
        @pl.loop(0, rows // high)
        def _(t):
            for r in range(0, high, 16):
                low = pl.multiple_of(t * high + r, 16)
                for i in range(0, order, wide):
                    total = body(pl.ds(low, 16), pl.ds(rows + low, 16), pl.ds(i, wide))
                    if stat is not None:
                        stats[stat, 0] += total

    def keep_data(real, imag, columns, xr, xi):
        vd[real, columns] = xr
        vd[imag, columns] = xi
        vd_turned[real, columns] = xi
        vd_turned[imag, columns] = -xr

    def keep_model(real, imag, columns, xr, xi):
        va[real, columns] = xr
        va[imag, columns] = xi
        va_turned[real, columns] = -xi
        va_turned[imag, columns] = xr

    def first_pass(real, imag, columns):
        xr, xi = vd[real, columns], vd[imag, columns]
        vd_turned[real, columns] = xi
        vd_turned[imag, columns] = -xr
        xr, xi = xr.astype(F32), xi.astype(F32)
        return fold(xr * xr + xi * xi)

    sweep(first_pass, 0)
    start_sum()
    for h in range(1, parts):
        for p in range(2):
            spread(z, h, p, True, True)

    @pl.loop(0, count)
    def _(i):
        work[:, block(i)] = jnp.zeros((2 * rows, wide), F32)

    beta = jnp.sqrt(finish_sum())
    inv_first = 1.0 / beta

    def forward_fit(low, columns):
        return dot(va[:, low], full[0, low, columns]) + dot(va_turned[:, low], full[1, low, columns])

    def adjoint_fit(band):
        return dot_t(vd[...], full[0, band, :]) + dot_t(vd_turned[...], full[1, band, :])

    def band_fit(v, p, band):
        return jnp.concatenate(
            [dot_t(v[r : r + rows], full[p, band, :]) for r in (0, rows)], axis=0
        )

    def begin(u):
        band = pl.ds(pl.multiple_of(u * unit, unit), unit)
        early[...] = band_fit(vd, 0, band)

    def process(u, split=False):
        band = pl.ds(pl.multiple_of(u * unit, unit), unit)
        slices = band_columns(u)
        fit = early[...] if split else band_fit(vd, 0, band)
        fit += band_fit(vd_turned, 1, band)
        width = unit // len(slices)
        total = jnp.zeros((8, 128), F32)
        for r in range(0, rows, 16):
            pair = pl.ds(r, 16), pl.ds(rows + r, 16)
            rounded = []
            for side in pair:
                pieces = []
                for k, columns in enumerate(slices):
                    x = fit[side.start : side.start + 16, k * width : (k + 1) * width]
                    x = (vd[side, columns].astype(F32) - weight * x) * inv_first
                    m_raw[side, columns] = x
                    work[side, columns] += x
                    total += fold(x * x)
                    pieces.append(x.astype(BF16))
                rounded.append(jnp.concatenate(pieces, axis=1))
            keep_model(*pair, band, *rounded)
        stats[1, 0] += total

        def visit(i):
            work[:, block(i)] -= weight * forward_fit(band, block(i))

        if split:
            for i in range(count):
                visit(i)
        else:
            pl.loop(0, count)(visit)

    def update_data(it, alpha, beta):
        inv_alpha, keep = 1.0 / alpha, alpha / beta

        def body(real, imag, columns):
            new = []
            for side in (real, imag):
                old = vd[side, columns].astype(F32) if it == 0 else d_raw[side, columns]
                new.append(work[side, columns] * inv_alpha - keep * old)
                d_raw[side, columns] = new[-1]
            keep_data(real, imag, columns, *[x.astype(BF16) for x in new])
            return fold(new[0] * new[0] + new[1] * new[1])

        sweep(body, 2 * it + 2)

    @pl.loop(0, m - 1 if shadow else m)
    def _(s):
        for h in range(parts):
            @pl.when(s > 0)
            def _():
                for p in range(2):
                    @pl.when(z - s >= 0)
                    def _():
                        await_piece(z - s, c, h, p)
                        spread(z - s, h, p, True, False)

                    @pl.when(z + s < m)
                    def _():
                        await_piece(z + s, c, h, p)
                        spread(z + s, h, p, False, True)

            @pl.loop(0, 2)
            def _(up):
                zb = z - s + 2 * s * up

                @pl.when((zb >= 0) & (zb < m) & ((s > 0) | (up == 0)))
                def _():
                    for p in range(2):
                        await_piece(zb, 1 - c, h, p)
                    if overlap:
                        process(zb * parts + h)

    if not overlap:
        @pl.loop(0, order // unit)
        def _(u):
            process(u)

    if shadow:
        @pl.when(jnp.logical_not(edge))
        def _():
            @pl.when((z == 1) | (z == m - 2))
            def _():
                home = jnp.where(z == 1, 0, m - 1)
                if parts == 1:
                    mine = [(home * 2 + c) * rows]
                    high = rows
                else:
                    mine = [(home * parts + c) * unit]
                    high = unit
                mine = [pl.ds(pl.multiple_of(x, high), high) for x in mine]
                for low in mine:
                    @pl.loop(0, order // unit)
                    def _(u):
                        band = pl.ds(pl.multiple_of(u * unit, unit), unit)
                        slices = band_columns(u)
                        for p in range(2):
                            fit = dot_t(full[p, low, :], full[0, band, :])
                            other = dot_t(full[1 - p, low, :], full[1, band, :])
                            fit = fit - other if p else fit + other
                            x = jnp.concatenate([full[p, low, s] for s in slices], axis=1)
                            raw = (x.astype(F32) - weight * fit) * inv_first
                            stats[1, 0] += fold(raw * raw)

            start_cast(0)

        @pl.when(edge)
        def _():
            zb = m - 1 - z
            for h in range(parts):
                u = zb * parts + h
                for p in range(2):
                    await_piece(zb, c, h, p)
                    block_copy(2, zb, c, h, p, sibling).start()
                    await_piece(zb, 1 - c, h, p)
                    if p == 0 and h == parts - 1:
                        begin(u)
                process(u, h == parts - 1)
    else:
        start_cast(0)

    alpha = jnp.sqrt(finish_cast(0, voters)[0])
    phi_bar, rho_bar = beta, alpha
    direction, answer = [1.0 / alpha], []
    everyone = range(n)
    for it in range(ITERS):
        last = it == ITERS - 1
        ka, kb = 2 * it, 2 * it + 1
        model_ref = models[it]

        if it > 0:
            @pl.loop(0, count)
            def _(i):
                fit = forward_fit(pl.ds(0, order), block(i))
                work[:, block(i)] = model_ref[:, block(i)] - weight * fit

            alpha = jnp.sqrt(finish_cast(ka, everyone)[0])
            rotate(alpha)
        update_data(it, alpha, beta)
        start_cast(kb)

        @pl.loop(0, count)
        def _(i):
            image[:, block(i)] = d_raw[:, block(i)] - weight * regroup(adjoint_fit(block(i)))

        if last:
            def squares(real, imag, columns):
                xr, xi = image[real, columns], image[imag, columns]
                return fold(xr * xr + xi * xi)

            def products(real, imag, columns):
                stats[kb + 2, 1] += fold(
                    image[real, columns] * model_ref[real, columns]
                    + image[imag, columns] * model_ref[imag, columns]
                )
                return squares(real, imag, columns)

            sweep(products, kb + 2)
            start_cast(kb + 1)

        data_sq = finish_cast(kb, everyone)[0]
        beta = jnp.sqrt(data_sq)
        inv_beta, shift = 1.0 / beta, beta / alpha

        if not last:
            def update_model(real, imag, columns):
                new = []
                for side in (real, imag):
                    new.append(image[side, columns] * inv_beta - shift * model_ref[side, columns])
                    models[it + 1][side, columns] = new[-1]
                keep_model(real, imag, columns, *[regroup(x.astype(BF16)) for x in new])
                return fold(new[0] * new[0] + new[1] * new[1])

            sweep(update_model, kb + 2)
            start_cast(kb + 1)

        rho = jnp.sqrt(rho_bar * rho_bar + beta * beta)
        cosine, sine = rho_bar / rho, beta / rho
        step = cosine * phi_bar / rho
        phi_bar = sine * phi_bar
        answer = [x + step * w for x, w in zip(answer + [0.0], direction)]

        def rotate(alpha, sine=sine, cosine=cosine, rho=rho):
            nonlocal rho_bar, direction
            rho_bar = -cosine * alpha
            turn = sine * alpha / rho
            direction = [-turn * w for w in direction] + [1.0 / alpha]

    def combine_basis(real, imag, columns):
        for side in (real, imag):
            basis = [model[side, columns] for model in models]
            fresh = image[side, columns]
            models[0][side, columns] = sum(w * x for w, x in zip(answer[1:], basis[1:])) + answer[0] * basis[0]
            models[1][side, columns] = sum(w * x for w, x in zip(direction[1:], basis[1:])) + direction[0] * basis[0]
            image[side, columns] = inv_beta * fresh - shift * basis[-1]

    sweep(combine_basis, None)
    drain_sum()
    pl.when(votes)(lambda: drain_cast(0))
    for k in range(1, 2 * ITERS):
        drain_cast(k)

    settle()

    image_sq, cross = finish_cast(2 * ITERS, everyone)
    new_alpha = jnp.sqrt(image_sq / data_sq - 2.0 * cross / alpha + data_sq)
    coef[0:1, :] = jnp.broadcast_to(-sine * new_alpha / rho, (1, 128))
    coef[1:2, :] = jnp.broadcast_to(1.0 / new_alpha, (1, 128))
    drain_cast(2 * ITERS)


def combine(coef, ready, turned, fresh, answer, direction, staged, sem):
    rows, order = answer.shape[2], answer.shape[3]
    high = min(rows, 64)
    per = rows // high

    def leave(o, p, i):
        source, out = ((ready, answer), (staged, direction))[o]
        return pltpu.make_async_copy(
            source.at[pl.ds(p * rows + i * high, high), :],
            out.at[0, p, pl.ds(i * high, high), :],
            sem.at[o, p, i],
        )

    tiles = [(p, i) for p in range(2) for i in range(per)]
    for p, i in tiles:
        leave(0, p, i).start()
    old, new = coef[0:1, 0:1], coef[1:2, 0:1]
    for p, i in tiles:
        band = pl.ds(p * rows + i * high, high)
        staged[band, :] = old * turned[band, :] + new * fresh[band, :]
        leave(1, p, i).start()
    for p, i in tiles:
        for o in range(2):
            leave(o, p, i).wait()


def on_device(n, nf, data):
    rows, order = data.shape[2], data.shape[3]
    weight = 1.0 / (3.0 * (2.0 * order) ** 0.5)
    wide, parts = block_sizes(rows, order)
    unit = 2 * rows // parts if rows % 128 == 0 else min(order, 256)
    field = pltpu.VMEM((2 * rows, order), F32)
    rounded = pltpu.VMEM((2 * rows, order), BF16)
    tile = pltpu.VMEM((8, 128), F32)
    casts = 1 + 2 * ITERS
    dma = pltpu.SemaphoreType.DMA
    vmem = pl.BlockSpec(memory_space=pltpu.VMEM)
    anywhere = pl.BlockSpec(memory_space=pl.ANY)
    *basis, coef = pl.pallas_call(
        functools.partial(kernel, n, nf, weight),
        out_shape=(field,) * (ITERS + 1) + (tile,),
        in_specs=[anywhere],
        out_specs=(vmem,) * (ITERS + 2),
        scratch_shapes=[
            pltpu.VMEM((2, order, order), BF16),
            rounded, rounded, rounded, rounded, field, field,
            pltpu.VMEM((2 * rows, unit), F32),
            pltpu.VMEM((casts + 1, 2, 8, 128), F32),
            pltpu.VMEM((n, 8, 128), F32), tile, pltpu.VMEM((nf, 8, 128), F32),
            pltpu.VMEM((casts, 1, 128), F32), pltpu.VMEM((casts, n * nf, 1, 128), F32),
            dma((2 * parts + 2,)), dma((3,)), dma((n, parts, 2)),
            dma((4,)), dma((casts,)), dma((casts,)),
        ],
        compiler_params=pltpu.CompilerParams(
            collective_id=0, has_side_effects=True, vmem_limit_bytes=46 * 2**20
        ),
    )(data)
    out = jax.ShapeDtypeStruct(data.shape, F32)
    high = min(rows, 64)
    return pl.pallas_call(
        combine,
        out_shape=(out, out),
        in_specs=[vmem] * (ITERS + 2),
        out_specs=(anywhere, anywhere),
        scratch_shapes=[pltpu.VMEM((2 * rows, order), F32), dma((2, 2, rows // high))],
        compiler_params=pltpu.CompilerParams(vmem_limit_bytes=24 * 2**20),
    )(coef, *basis)


def solution(mesh):
    spec = P("freq", None, "row", None)
    return jax.shard_map(
        functools.partial(on_device, mesh.shape["row"], mesh.shape["freq"]),
        mesh=mesh,
        in_specs=(spec,),
        out_specs=(spec, spec),
        check_vma=False,
    )
```

```python
import functools

import jax
import jax.numpy as jnp
from jax import lax
from jax.experimental import pallas as pl
from jax.experimental.pallas import tpu as pltpu
from jax.sharding import PartitionSpec as P

ITERS = 2
MESH = pl.DeviceIdType.MESH
F32 = jnp.float32
BF16 = jnp.bfloat16


def dot(a, b):
    return lax.dot_general(a, b, (((1,), (0,)), ((), ())), preferred_element_type=F32)


def dot_t(a, b):
    return lax.dot_general(a, b, (((1,), (1,)), ((), ())), preferred_element_type=F32)


def fold(x):
    tiles = [
        x[r : r + 8, i : i + 128]
        for r in range(0, x.shape[0], 8)
        for i in range(0, x.shape[1], 128)
    ]
    while len(tiles) > 1:
        tiles = [sum(tiles[k : k + 2][1:], tiles[k]) for k in range(0, len(tiles), 2)]
    return tiles[0]


def block_sizes(rows, order):
    wide = min(order // 2, 512)
    return wide, 2 if rows % 256 == 0 and wide % (2 * rows) == 0 else 1


def kernel(
    n, nf, weight, data, *refs,
):
    models, image, coef, refs = refs[:ITERS], refs[ITERS], refs[ITERS + 1], refs[ITERS + 2 :]
    (
        full, va, vd, va_turned, vd_turned, d_raw, work, early,
        stats, slots, sums, fslots, spot, seats,
        load_sem, ssem, rsem, sum_sem, cast_s, cast_r,
    ) = refs
    m_raw = models[0]
    rows, order = data.shape[2], data.shape[3]
    m = n // 2
    me = lax.axis_index("row")
    mf = lax.axis_index("freq")
    z, c = lax.div(me, 2), lax.rem(me, 2)
    sibling = z * 2 + (1 - c)
    wide, parts = block_sizes(rows, order)
    half = rows // parts
    count = order // wide
    overlap = rows % 128 == 0
    unit = 2 * half if overlap else min(order, 256)
    shadow = overlap and m >= 4
    edge = (z == 0) | (z == m - 1)
    voters = range(2, n - 2) if shadow else range(n)
    votes = (me >= voters[0]) & (me <= voters[-1])

    def at_row(r):
        return {"row": r}

    def wrap(x, size):
        return jnp.where(x >= size, x - size, x)

    def block(i):
        return pl.ds(pl.multiple_of(i * wide, wide), wide)

    def piece(zb, cc, h, p):
        start = pl.multiple_of(((zb * parts + h) * 2 + cc) * half, half)
        return full.at[p, pl.ds(start, half), :]

    def band_columns(u):
        if parts == 1:
            return [pl.ds(pl.multiple_of(u * unit, unit), unit)]
        base = lax.div(u, 2) * 2 * rows + lax.rem(u, 2) * half
        return [pl.ds(pl.multiple_of(base + cc * rows, half), half) for cc in range(2)]

    def regroup(x):
        if parts == 1:
            return x
        group = 2 * rows
        return jnp.concatenate(
            [
                x[:, g + k * half : g + (k + 1) * half]
                for g in range(0, x.shape[1], group)
                for k in (0, 2, 1, 3)
            ],
            axis=1,
        )

    loads = []
    for h in range(parts):
        for p in range(2):
            loads.append(
                pltpu.make_async_copy(
                    data.at[0, p, pl.ds(h * half, half), :],
                    piece(z, c, h, p), load_sem.at[h * 2 + p],
                )
            )
    for p in range(2):
        loads.append(
            pltpu.make_async_copy(
                data.at[0, p], vd.at[pl.ds(p * rows, rows), :], load_sem.at[2 * parts + p]
            )
        )
    for copy in loads:
        copy.start()

    barrier = pltpu.get_barrier_semaphore()

    @pl.loop(1, n)
    def _(k):
        pl.semaphore_signal(
            barrier, inc=1, device_id=at_row(wrap(me + k, n)), device_id_type=MESH
        )

    @pl.loop(1, nf)
    def _(k):
        pl.semaphore_signal(
            barrier, inc=1, device_id={"freq": wrap(mf + k, nf)}, device_id_type=MESH
        )

    stats[...] = jnp.zeros_like(stats)
    for copy in loads[: 2 * parts]:
        copy.wait()
    pl.semaphore_wait(barrier, n - 1 + nf - 1)

    def row_stat(j, seat):
        return pltpu.make_async_remote_copy(
            src_ref=stats.at[0, 0], dst_ref=slots.at[seat], send_sem=sum_sem.at[0],
            recv_sem=sum_sem.at[1], device_id=at_row(j), device_id_type=MESH,
        )

    def freq_stat(j, seat):
        return pltpu.make_async_remote_copy(
            src_ref=sums, dst_ref=fslots.at[seat], send_sem=sum_sem.at[2],
            recv_sem=sum_sem.at[3], device_id={"freq": j}, device_id_type=MESH,
        )

    def bulk(ref, send_sem, recv_sem):
        return pltpu.make_async_remote_copy(
            src_ref=ref, dst_ref=ref, send_sem=send_sem, recv_sem=recv_sem,
            device_id=at_row(sibling), device_id_type=MESH,
        )

    def rows_bulk():
        return bulk(slots.at[pl.ds(0, n - 1)], sum_sem.at[0], sum_sem.at[1])

    def freqs_bulk():
        return bulk(fslots.at[pl.ds(0, nf - 1)], sum_sem.at[2], sum_sem.at[3])

    def start_sum():
        slots[me] = stats[0, 0]

        @pl.loop(1, n)
        def _(i):
            row_stat(wrap(me + i, n), me).start()

    def finish_sum():
        rows_bulk().wait_recv()
        total = jnp.sum(slots[...], axis=0)
        sums[...] = total
        fslots[mf] = total

        @pl.loop(1, nf)
        def _(i):
            freq_stat(wrap(mf + i, nf), mf).start()

        freqs_bulk().wait_recv()
        total = jnp.sum(jnp.sum(fslots[...], axis=0), axis=0, keepdims=True)
        return jnp.sum(total, axis=1, keepdims=True)

    def drain_sum():
        rows_bulk().wait_send()
        freqs_bulk().wait_send()

    def cast(k, j, g):
        return pltpu.make_async_remote_copy(
            src_ref=spot.at[k], dst_ref=seats.at[k, me * nf + mf],
            send_sem=cast_s.at[k], recv_sem=cast_r.at[k],
            device_id={"row": j, "freq": g}, device_id_type=MESH,
        )

    def cast_bulk(k, number):
        return bulk(seats.at[k, pl.ds(0, number)], cast_s.at[k], cast_r.at[k])

    def others(body):
        if n * nf <= 64:
            for i in range(n):
                for e in range(nf):
                    if i or e:
                        body(wrap(me + i, n), wrap(mf + e, nf))
            return

        @pl.loop(0, n)
        def _(i):
            j = wrap(me + i, n)
            pl.when(i > 0)(lambda: body(j, mf))
            for e in range(1, nf):
                body(j, wrap(mf + e, nf))

    def start_cast(k):
        first, second = [
            jnp.sum(jnp.sum(stats[k + 1, q], axis=0, keepdims=True), axis=1, keepdims=True)
            for q in range(2)
        ]
        lane = lax.broadcasted_iota(jnp.int32, (1, 128), 1)
        spot[k] = jnp.where(lane < 64, first, second)
        seats[k, me * nf + mf] = spot[k]
        others(lambda j, g: cast(k, j, g).start())

    def finish_cast(k, members):
        number = len(members) * nf
        if number == n * nf:
            cast_bulk(k, number - 1).wait_recv()
        else:
            pl.when(votes)(lambda: cast_bulk(k, number - 1).wait_recv())
            pl.when(jnp.logical_not(votes))(lambda: cast_bulk(k, number).wait_recv())

        held = seats[k, members[0] * nf : (members[-1] + 1) * nf]
        total = jnp.sum(held, axis=0)
        return total[:, 0:1], total[:, 64:65]

    def drain_cast(k):
        cast_bulk(k, n * nf - 1).wait_send()

    def block_copy(lane, zb, cc, h, p, target):
        return pltpu.make_async_remote_copy(
            src_ref=piece(zb, cc, h, p), dst_ref=piece(zb, cc, h, p),
            send_sem=ssem.at[lane], recv_sem=rsem.at[zb * 2 + cc, h, p],
            device_id=at_row(target), device_id_type=MESH,
        )

    above_me, below_me = wrap(me + 2, n), wrap(me + n - 2, n)

    def spread(zb, h, p, up, down):
        if up:
            @pl.when(z + 1 < m)
            def _():
                block_copy(0, zb, c, h, p, above_me).start()

        if down:
            @pl.when(z > 0)
            def _():
                block_copy(1, zb, c, h, p, below_me).start()

        block_copy(2, zb, c, h, p, sibling).start()

    def settle():
        def sent(lane, blocks):
            bulk(full.at[0, pl.ds(0, 2 * rows * blocks), :], ssem.at[lane], ssem.at[lane]).wait_send()

        for k in range(m):
            @pl.when(z == k)
            def _():
                if k < m - 1:
                    sent(0, k + 1)
                if k > 0:
                    sent(1, m - k)

        sent(2, m)

    def await_piece(zb, cc, h, p):
        block_copy(0, zb, cc, h, p, sibling).wait_recv()

    for p in range(2):
        spread(z, 0, p, True, True)
    for copy in loads[2 * parts :]:
        copy.wait()

    high = 64 if rows % 64 == 0 else 16

    def tiles(body, stat, done):
        for i in done:
            total = jnp.zeros((8, 128), F32)
            for r in range(0, rows, 16):
                part = body(pl.ds(r, 16), pl.ds(rows + r, 16), pl.ds(i * wide, wide))
                total += part
            stats[stat, 0] += total

    def sweep(body, stat):
        @pl.loop(0, rows // high)
        def _(t):
            for r in range(0, high, 16):
                low = pl.multiple_of(t * high + r, 16)
                for i in range(0, order, wide):
                    total = body(pl.ds(low, 16), pl.ds(rows + low, 16), pl.ds(i, wide))
                    if stat is not None:
                        stats[stat, 0] += total

    def keep_data(real, imag, columns, xr, xi):
        vd[real, columns] = xr
        vd[imag, columns] = xi
        vd_turned[real, columns] = xi
        vd_turned[imag, columns] = -xr

    def keep_model(real, imag, columns, xr, xi):
        va[real, columns] = xr
        va[imag, columns] = xi
        va_turned[real, columns] = -xi
        va_turned[imag, columns] = xr

    def first_pass(real, imag, columns):
        xr, xi = vd[real, columns], vd[imag, columns]
        vd_turned[real, columns] = xi
        vd_turned[imag, columns] = -xr
        xr, xi = xr.astype(F32), xi.astype(F32)
        return fold(xr * xr + xi * xi)

    sweep(first_pass, 0)
    start_sum()
    for h in range(1, parts):
        for p in range(2):
            spread(z, h, p, True, True)

    @pl.loop(0, count)
    def _(i):
        work[:, block(i)] = jnp.zeros((2 * rows, wide), F32)

    beta = jnp.sqrt(finish_sum())
    inv_first = 1.0 / beta

    def forward_fit(low, columns):
        return dot(va[:, low], full[0, low, columns]) + dot(va_turned[:, low], full[1, low, columns])

    def adjoint_fit(band):
        return dot_t(vd[...], full[0, band, :]) + dot_t(vd_turned[...], full[1, band, :])

    def band_fit(v, p, band):
        return jnp.concatenate(
            [dot_t(v[r : r + rows], full[p, band, :]) for r in (0, rows)], axis=0
        )

    def begin(u):
        band = pl.ds(pl.multiple_of(u * unit, unit), unit)
        early[...] = band_fit(vd, 0, band)

    def process(u, split=False):
        band = pl.ds(pl.multiple_of(u * unit, unit), unit)
        slices = band_columns(u)
        fit = early[...] if split else band_fit(vd, 0, band)
        fit += band_fit(vd_turned, 1, band)
        width = unit // len(slices)
        total = jnp.zeros((8, 128), F32)
        for r in range(0, rows, 16):
            pair = pl.ds(r, 16), pl.ds(rows + r, 16)
            rounded = []
            for side in pair:
                pieces = []
                for k, columns in enumerate(slices):
                    x = fit[side.start : side.start + 16, k * width : (k + 1) * width]
                    x = (vd[side, columns].astype(F32) - weight * x) * inv_first
                    m_raw[side, columns] = x
                    work[side, columns] += x
                    total += fold(x * x)
                    pieces.append(x.astype(BF16))
                rounded.append(jnp.concatenate(pieces, axis=1))
            keep_model(*pair, band, *rounded)
        stats[1, 0] += total

        def visit(i):
            work[:, block(i)] -= weight * forward_fit(band, block(i))

        if split:
            for i in range(count):
                visit(i)
        else:
            pl.loop(0, count)(visit)

    def update_data(it, alpha, beta):
        inv_alpha, keep = 1.0 / alpha, alpha / beta

        def body(real, imag, columns):
            new = []
            for side in (real, imag):
                old = vd[side, columns].astype(F32) if it == 0 else d_raw[side, columns]
                new.append(work[side, columns] * inv_alpha - keep * old)
                d_raw[side, columns] = new[-1]
            keep_data(real, imag, columns, *[x.astype(BF16) for x in new])
            return fold(new[0] * new[0] + new[1] * new[1])

        return body

    @pl.loop(0, m - 1 if shadow else m)
    def _(s):
        for h in range(parts):
            @pl.when(s > 0)
            def _():
                for p in range(2):
                    @pl.when(z - s >= 0)
                    def _():
                        await_piece(z - s, c, h, p)
                        spread(z - s, h, p, True, False)

                    @pl.when(z + s < m)
                    def _():
                        await_piece(z + s, c, h, p)
                        spread(z + s, h, p, False, True)

            @pl.loop(0, 2)
            def _(up):
                zb = z - s + 2 * s * up

                @pl.when((zb >= 0) & (zb < m) & ((s > 0) | (up == 0)))
                def _():
                    for p in range(2):
                        await_piece(zb, 1 - c, h, p)
                    if overlap:
                        process(zb * parts + h)

    if not overlap:
        @pl.loop(0, order // unit)
        def _(u):
            process(u)

    if shadow:
        @pl.when(jnp.logical_not(edge))
        def _():
            @pl.when((z == 1) | (z == m - 2))
            def _():
                home = jnp.where(z == 1, 0, m - 1)
                if parts == 1:
                    mine = [(home * 2 + c) * rows]
                    high = rows
                else:
                    mine = [(home * parts + c) * unit]
                    high = unit
                mine = [pl.ds(pl.multiple_of(x, high), high) for x in mine]
                for low in mine:
                    @pl.loop(0, order // unit)
                    def _(u):
                        band = pl.ds(pl.multiple_of(u * unit, unit), unit)
                        slices = band_columns(u)
                        for p in range(2):
                            fit = dot_t(full[p, low, :], full[0, band, :])
                            other = dot_t(full[1 - p, low, :], full[1, band, :])
                            fit = fit - other if p else fit + other
                            x = jnp.concatenate([full[p, low, s] for s in slices], axis=1)
                            raw = (x.astype(F32) - weight * fit) * inv_first
                            stats[1, 0] += fold(raw * raw)

            start_cast(0)

        @pl.when(edge)
        def _():
            zb = m - 1 - z
            for h in range(parts):
                u = zb * parts + h
                for p in range(2):
                    await_piece(zb, c, h, p)
                    block_copy(2, zb, c, h, p, sibling).start()
                    await_piece(zb, 1 - c, h, p)
                    if p == 0 and h == parts - 1:
                        begin(u)
                process(u, h == parts - 1)
    else:
        start_cast(0)

    alpha = jnp.sqrt(finish_cast(0, voters)[0])
    phi_bar, rho_bar = beta, alpha
    direction, answer = [1.0 / alpha], []
    everyone = range(n)
    for it in range(ITERS):
        last = it == ITERS - 1
        ka, kb = 2 * it, 2 * it + 1
        model_ref = models[it]

        def forward_block(i):
            fit = forward_fit(pl.ds(0, order), block(i))
            work[:, block(i)] = model_ref[:, block(i)] - weight * fit

        def adjoint_block(i):
            image[:, block(i)] = d_raw[:, block(i)] - weight * regroup(adjoint_fit(block(i)))

        if it > 0:
            for i in range(count - 1):
                forward_block(i)
            alpha = jnp.sqrt(finish_cast(ka, everyone)[0])
            rotate(alpha)
            body = update_data(it, alpha, beta)
            tiles(body, kb + 1, range(count - 1))
            forward_block(count - 1)
            tiles(body, kb + 1, range(count - 1, count))
        else:
            sweep(update_data(it, alpha, beta), kb + 1)
        start_cast(kb)

        if last:
            def products(real, imag, columns):
                xr, xi = image[real, columns], image[imag, columns]
                stats[kb + 2, 1] += fold(xr * model_ref[real, columns] + xi * model_ref[imag, columns])
                return fold(xr * xr + xi * xi)

            for i in range(count):
                adjoint_block(i)
                tiles(products, kb + 2, range(i - 1, i) if i else ())
            tiles(products, kb + 2, range(count - 1, count))
            start_cast(kb + 1)
        else:
            for i in range(count - 1):
                adjoint_block(i)

        data_sq = finish_cast(kb, everyone)[0]
        beta = jnp.sqrt(data_sq)
        inv_beta, shift = 1.0 / beta, beta / alpha

        if not last:
            def update_model(real, imag, columns):
                new = []
                for side in (real, imag):
                    new.append(image[side, columns] * inv_beta - shift * model_ref[side, columns])
                    models[it + 1][side, columns] = new[-1]
                keep_model(real, imag, columns, *[regroup(x.astype(BF16)) for x in new])
                return fold(new[0] * new[0] + new[1] * new[1])

            tiles(update_model, kb + 2, range(count - 1))
            adjoint_block(count - 1)
            tiles(update_model, kb + 2, range(count - 1, count))
            start_cast(kb + 1)

        rho = jnp.sqrt(rho_bar * rho_bar + beta * beta)
        cosine, sine = rho_bar / rho, beta / rho
        step = cosine * phi_bar / rho
        phi_bar = sine * phi_bar
        answer = [x + step * w for x, w in zip(answer + [0.0], direction)]

        def rotate(alpha, sine=sine, cosine=cosine, rho=rho):
            nonlocal rho_bar, direction
            rho_bar = -cosine * alpha
            turn = sine * alpha / rho
            direction = [-turn * w for w in direction] + [1.0 / alpha]

    def combine_basis(real, imag, columns):
        for side in (real, imag):
            basis = [model[side, columns] for model in models]
            fresh = image[side, columns]
            models[0][side, columns] = sum(w * x for w, x in zip(answer[1:], basis[1:])) + answer[0] * basis[0]
            models[1][side, columns] = sum(w * x for w, x in zip(direction[1:], basis[1:])) + direction[0] * basis[0]
            image[side, columns] = inv_beta * fresh - shift * basis[-1]

    sweep(combine_basis, None)
    drain_sum()
    pl.when(votes)(lambda: drain_cast(0))
    for k in range(1, 2 * ITERS):
        drain_cast(k)

    settle()

    image_sq, cross = finish_cast(2 * ITERS, everyone)
    new_alpha = jnp.sqrt(image_sq / data_sq - 2.0 * cross / alpha + data_sq)
    coef[0:1, :] = jnp.broadcast_to(-sine * new_alpha / rho, (1, 128))
    coef[1:2, :] = jnp.broadcast_to(1.0 / new_alpha, (1, 128))
    drain_cast(2 * ITERS)


def combine(coef, ready, turned, fresh, answer, direction, staged, sem):
    rows, order = answer.shape[2], answer.shape[3]
    high = min(rows, 64)
    per = rows // high

    def leave(o, p, i):
        source, out = ((ready, answer), (staged, direction))[o]
        return pltpu.make_async_copy(
            source.at[pl.ds(p * rows + i * high, high), :],
            out.at[0, p, pl.ds(i * high, high), :],
            sem.at[o, p, i],
        )

    tiles = [(p, i) for p in range(2) for i in range(per)]
    for p, i in tiles:
        leave(0, p, i).start()
    old, new = coef[0:1, 0:1], coef[1:2, 0:1]
    for p, i in tiles:
        band = pl.ds(p * rows + i * high, high)
        staged[band, :] = old * turned[band, :] + new * fresh[band, :]
        leave(1, p, i).start()
    for p, i in tiles:
        for o in range(2):
            leave(o, p, i).wait()


def on_device(n, nf, data):
    rows, order = data.shape[2], data.shape[3]
    weight = 1.0 / (3.0 * (2.0 * order) ** 0.5)
    wide, parts = block_sizes(rows, order)
    unit = 2 * rows // parts if rows % 128 == 0 else min(order, 256)
    field = pltpu.VMEM((2 * rows, order), F32)
    rounded = pltpu.VMEM((2 * rows, order), BF16)
    tile = pltpu.VMEM((8, 128), F32)
    casts = 1 + 2 * ITERS
    dma = pltpu.SemaphoreType.DMA
    vmem = pl.BlockSpec(memory_space=pltpu.VMEM)
    anywhere = pl.BlockSpec(memory_space=pl.ANY)
    *basis, coef = pl.pallas_call(
        functools.partial(kernel, n, nf, weight),
        out_shape=(field,) * (ITERS + 1) + (tile,),
        in_specs=[anywhere],
        out_specs=(vmem,) * (ITERS + 2),
        scratch_shapes=[
            pltpu.VMEM((2, order, order), BF16),
            rounded, rounded, rounded, rounded, field, field,
            pltpu.VMEM((2 * rows, unit), F32),
            pltpu.VMEM((casts + 1, 2, 8, 128), F32),
            pltpu.VMEM((n, 8, 128), F32), tile, pltpu.VMEM((nf, 8, 128), F32),
            pltpu.VMEM((casts, 1, 128), F32), pltpu.VMEM((casts, n * nf, 1, 128), F32),
            dma((2 * parts + 2,)), dma((3,)), dma((n, parts, 2)),
            dma((4,)), dma((casts,)), dma((casts,)),
        ],
        compiler_params=pltpu.CompilerParams(
            collective_id=0, has_side_effects=True, vmem_limit_bytes=46 * 2**20
        ),
    )(data)
    out = jax.ShapeDtypeStruct(data.shape, F32)
    high = min(rows, 64)
    return pl.pallas_call(
        combine,
        out_shape=(out, out),
        in_specs=[vmem] * (ITERS + 2),
        out_specs=(anywhere, anywhere),
        scratch_shapes=[pltpu.VMEM((2 * rows, order), F32), dma((2, 2, rows // high))],
        compiler_params=pltpu.CompilerParams(vmem_limit_bytes=24 * 2**20),
    )(coef, *basis)


def solution(mesh):
    spec = P("freq", None, "row", None)
    return jax.shard_map(
        functools.partial(on_device, mesh.shape["row"], mesh.shape["freq"]),
        mesh=mesh,
        in_specs=(spec,),
        out_specs=(spec, spec),
        check_vma=False,
    )
```

```python
import functools

import jax
import jax.numpy as jnp
from jax import lax
from jax.experimental import pallas as pl
from jax.experimental.pallas import tpu as pltpu
from jax.sharding import PartitionSpec as P

ITERS = 2
MESH = pl.DeviceIdType.MESH
F32 = jnp.float32
BF16 = jnp.bfloat16


def dot(a, b):
    return lax.dot_general(a, b, (((1,), (0,)), ((), ())), preferred_element_type=F32)


def dot_t(a, b):
    return lax.dot_general(a, b, (((1,), (1,)), ((), ())), preferred_element_type=F32)


def fold(x):
    tiles = [
        x[r : r + 8, i : i + 128]
        for r in range(0, x.shape[0], 8)
        for i in range(0, x.shape[1], 128)
    ]
    while len(tiles) > 1:
        tiles = [sum(tiles[k : k + 2][1:], tiles[k]) for k in range(0, len(tiles), 2)]
    return tiles[0]


def block_sizes(rows, order):
    wide = min(order // 2, 512)
    return wide, 2 if rows % 256 == 0 and wide % (2 * rows) == 0 else 1


def kernel(
    n, nf, weight, data, *refs,
):
    models, image, coef, refs = refs[:ITERS], refs[ITERS], refs[ITERS + 1], refs[ITERS + 2 :]
    (
        full, va, vd, va_turned, vd_turned, d_raw, work, early,
        stats, slots, sums, fslots, spot, seats,
        load_sem, ssem, rsem, sum_sem, cast_s, cast_r,
    ) = refs
    m_raw = models[0]
    rows, order = data.shape[2], data.shape[3]
    m = n // 2
    me = lax.axis_index("row")
    mf = lax.axis_index("freq")
    z, c = lax.div(me, 2), lax.rem(me, 2)
    sibling = z * 2 + (1 - c)
    wide, parts = block_sizes(rows, order)
    half = rows // parts
    count = order // wide
    overlap = rows % 128 == 0
    unit = 2 * half if overlap else min(order, 256)
    shadow = overlap and m >= 4
    edge = (z == 0) | (z == m - 1)
    voters = range(2, n - 2) if shadow else range(n)
    votes = (me >= voters[0]) & (me <= voters[-1])

    def at_row(r):
        return {"row": r}

    def wrap(x, size):
        return jnp.where(x >= size, x - size, x)

    def block(i):
        return pl.ds(pl.multiple_of(i * wide, wide), wide)

    def piece(zb, cc, h, p):
        start = pl.multiple_of(((zb * parts + h) * 2 + cc) * half, half)
        return full.at[p, pl.ds(start, half), :]

    def band_columns(u):
        if parts == 1:
            return [pl.ds(pl.multiple_of(u * unit, unit), unit)]
        base = lax.div(u, 2) * 2 * rows + lax.rem(u, 2) * half
        return [pl.ds(pl.multiple_of(base + cc * rows, half), half) for cc in range(2)]

    def regroup(x):
        if parts == 1:
            return x
        group = 2 * rows
        return jnp.concatenate(
            [
                x[:, g + k * half : g + (k + 1) * half]
                for g in range(0, x.shape[1], group)
                for k in (0, 2, 1, 3)
            ],
            axis=1,
        )

    loads = []
    for h in range(parts):
        for p in range(2):
            loads.append(
                pltpu.make_async_copy(
                    data.at[0, p, pl.ds(h * half, half), :],
                    piece(z, c, h, p), load_sem.at[h * 2 + p],
                )
            )
    for p in range(2):
        loads.append(
            pltpu.make_async_copy(
                data.at[0, p], vd.at[pl.ds(p * rows, rows), :], load_sem.at[2 * parts + p]
            )
        )
    for copy in loads:
        copy.start()

    barrier = pltpu.get_barrier_semaphore()

    @pl.loop(1, n)
    def _(k):
        pl.semaphore_signal(
            barrier, inc=1, device_id=at_row(wrap(me + k, n)), device_id_type=MESH
        )

    @pl.loop(1, nf)
    def _(k):
        pl.semaphore_signal(
            barrier, inc=1, device_id={"freq": wrap(mf + k, nf)}, device_id_type=MESH
        )

    stats[...] = jnp.zeros_like(stats)
    for copy in loads[: 2 * parts]:
        copy.wait()
    pl.semaphore_wait(barrier, n - 1 + nf - 1)

    def row_stat(j, seat):
        return pltpu.make_async_remote_copy(
            src_ref=stats.at[0, 0], dst_ref=slots.at[seat], send_sem=sum_sem.at[0],
            recv_sem=sum_sem.at[1], device_id=at_row(j), device_id_type=MESH,
        )

    def freq_stat(j, seat):
        return pltpu.make_async_remote_copy(
            src_ref=sums, dst_ref=fslots.at[seat], send_sem=sum_sem.at[2],
            recv_sem=sum_sem.at[3], device_id={"freq": j}, device_id_type=MESH,
        )

    def bulk(ref, send_sem, recv_sem):
        return pltpu.make_async_remote_copy(
            src_ref=ref, dst_ref=ref, send_sem=send_sem, recv_sem=recv_sem,
            device_id=at_row(sibling), device_id_type=MESH,
        )

    def rows_bulk():
        return bulk(slots.at[pl.ds(0, n - 1)], sum_sem.at[0], sum_sem.at[1])

    def freqs_bulk():
        return bulk(fslots.at[pl.ds(0, nf - 1)], sum_sem.at[2], sum_sem.at[3])

    def start_sum():
        slots[me] = stats[0, 0]

        @pl.loop(1, n)
        def _(i):
            row_stat(wrap(me + i, n), me).start()

    def finish_sum():
        rows_bulk().wait_recv()
        total = jnp.sum(slots[...], axis=0)
        sums[...] = total
        fslots[mf] = total

        @pl.loop(1, nf)
        def _(i):
            freq_stat(wrap(mf + i, nf), mf).start()

        freqs_bulk().wait_recv()
        total = jnp.sum(jnp.sum(fslots[...], axis=0), axis=0, keepdims=True)
        return jnp.sum(total, axis=1, keepdims=True)

    def drain_sum():
        rows_bulk().wait_send()
        freqs_bulk().wait_send()

    def cast(k, j, g):
        return pltpu.make_async_remote_copy(
            src_ref=spot.at[k], dst_ref=seats.at[k, me * nf + mf],
            send_sem=cast_s.at[k], recv_sem=cast_r.at[k],
            device_id={"row": j, "freq": g}, device_id_type=MESH,
        )

    def cast_bulk(k, number):
        return bulk(seats.at[k, pl.ds(0, number)], cast_s.at[k], cast_r.at[k])

    def others(body):
        if n * nf <= 64:
            for i in sorted(range(n), key=lambda i: -abs(2 * i - n)):
                for e in reversed(range(nf)):
                    if i or e:
                        body(wrap(me + i, n), wrap(mf + e, nf))
            return

        @pl.loop(0, n)
        def _(i):
            j = wrap(me + i, n)
            pl.when(i > 0)(lambda: body(j, mf))
            for e in range(1, nf):
                body(j, wrap(mf + e, nf))

    def start_cast(k):
        first, second = [
            jnp.sum(jnp.sum(stats[k + 1, q], axis=0, keepdims=True), axis=1, keepdims=True)
            for q in range(2)
        ]
        lane = lax.broadcasted_iota(jnp.int32, (1, 128), 1)
        spot[k] = jnp.where(lane < 64, first, second)
        seats[k, me * nf + mf] = spot[k]
        others(lambda j, g: cast(k, j, g).start())

    def await_cast(k, members):
        number = len(members) * nf
        if number == n * nf:
            cast_bulk(k, number - 1).wait_recv()
        else:
            pl.when(votes)(lambda: cast_bulk(k, number - 1).wait_recv())
            pl.when(jnp.logical_not(votes))(lambda: cast_bulk(k, number).wait_recv())

    def read_cast(k, members):
        held = seats[k, members[0] * nf : (members[-1] + 1) * nf]
        total = jnp.sum(held, axis=0)
        return total[:, 0:1], total[:, 64:65]

    def finish_cast(k, members):
        await_cast(k, members)
        return read_cast(k, members)

    def drain_cast(k):
        cast_bulk(k, n * nf - 1).wait_send()

    def block_copy(lane, zb, cc, h, p, target):
        return pltpu.make_async_remote_copy(
            src_ref=piece(zb, cc, h, p), dst_ref=piece(zb, cc, h, p),
            send_sem=ssem.at[lane], recv_sem=rsem.at[zb * 2 + cc, h, p],
            device_id=at_row(target), device_id_type=MESH,
        )

    above_me, below_me = wrap(me + 2, n), wrap(me + n - 2, n)

    def spread(zb, h, p, up, down):
        if up:
            @pl.when(z + 1 < m)
            def _():
                block_copy(0, zb, c, h, p, above_me).start()

        if down:
            @pl.when(z > 0)
            def _():
                block_copy(1, zb, c, h, p, below_me).start()

        block_copy(2, zb, c, h, p, sibling).start()

    def settle():
        def sent(lane, blocks):
            bulk(full.at[0, pl.ds(0, 2 * rows * blocks), :], ssem.at[lane], ssem.at[lane]).wait_send()

        for k in range(m):
            @pl.when(z == k)
            def _():
                if k < m - 1:
                    sent(0, k + 1)
                if k > 0:
                    sent(1, m - k)

        sent(2, m)

    def await_piece(zb, cc, h, p):
        block_copy(0, zb, cc, h, p, sibling).wait_recv()

    for p in range(2):
        spread(z, 0, p, True, True)
    for copy in loads[2 * parts :]:
        copy.wait()

    high = 128 if rows % 128 == 0 else 16

    def tiles(body, stat, done):
        for i in done:
            total = jnp.zeros((8, 128), F32)
            for r in range(0, rows, 16):
                part = body(pl.ds(r, 16), pl.ds(rows + r, 16), pl.ds(i * wide, wide))
                total += part
            stats[stat, 0] += total

    def sweep(body, stat):
        @pl.loop(0, rows // high)
        def _(t):
            for r in range(0, high, 16):
                low = pl.multiple_of(t * high + r, 16)
                for i in range(0, order, wide):
                    total = body(pl.ds(low, 16), pl.ds(rows + low, 16), pl.ds(i, wide))
                    if stat is not None:
                        stats[stat, 0] += total

    def keep_data(real, imag, columns, xr, xi):
        vd[real, columns] = xr
        vd[imag, columns] = xi
        vd_turned[real, columns] = xi
        vd_turned[imag, columns] = -xr

    def keep_model(real, imag, columns, xr, xi):
        va[real, columns] = xr
        va[imag, columns] = xi
        va_turned[real, columns] = -xi
        va_turned[imag, columns] = xr

    def first_pass(real, imag, columns):
        xr, xi = vd[real, columns], vd[imag, columns]
        vd_turned[real, columns] = xi
        vd_turned[imag, columns] = -xr
        xr, xi = xr.astype(F32), xi.astype(F32)
        return fold(xr * xr + xi * xi)

    sweep(first_pass, 0)
    start_sum()
    for h in range(1, parts):
        for p in range(2):
            spread(z, h, p, True, True)

    @pl.loop(0, count)
    def _(i):
        work[:, block(i)] = jnp.zeros((2 * rows, wide), F32)

    beta = jnp.sqrt(finish_sum())
    inv_first = 1.0 / beta

    def forward_fit(low, columns):
        return dot(va[:, low], full[0, low, columns]) + dot(va_turned[:, low], full[1, low, columns])

    def adjoint_fit(band):
        return dot_t(vd[...], full[0, band, :]) + dot_t(vd_turned[...], full[1, band, :])

    def band_fit(v, p, band):
        return jnp.concatenate(
            [dot_t(v[r : r + rows], full[p, band, :]) for r in (0, rows)], axis=0
        )

    def begin(u):
        band = pl.ds(pl.multiple_of(u * unit, unit), unit)
        early[...] = band_fit(vd, 0, band)

    def process(u, split=False, after=None):
        band = pl.ds(pl.multiple_of(u * unit, unit), unit)
        slices = band_columns(u)
        fit = early[...] if split else band_fit(vd, 0, band)
        fit += band_fit(vd_turned, 1, band)
        width = unit // len(slices)
        total = jnp.zeros((8, 128), F32)
        for r in range(0, rows, 16):
            pair = pl.ds(r, 16), pl.ds(rows + r, 16)
            rounded = []
            for side in pair:
                pieces = []
                for k, columns in enumerate(slices):
                    x = fit[side.start : side.start + 16, k * width : (k + 1) * width]
                    x = (vd[side, columns].astype(F32) - weight * x) * inv_first
                    m_raw[side, columns] = x
                    work[side, columns] += x
                    total += fold(x * x)
                    pieces.append(x.astype(BF16))
                rounded.append(jnp.concatenate(pieces, axis=1))
            keep_model(*pair, band, *rounded)
        stats[1, 0] += total

        def visit(i):
            work[:, block(i)] -= weight * forward_fit(band, block(i))

        if split:
            for i in range(count):
                visit(i)
                if i:
                    tiles(after, 2, range(i - 1, i))
            tiles(after, 2, range(count - 1, count))
        else:
            pl.loop(0, count)(visit)

    def update_data(it, alpha, beta):
        inv_alpha, keep = 1.0 / alpha, alpha / beta

        def body(real, imag, columns):
            new = []
            for side in (real, imag):
                old = vd[side, columns].astype(F32) if it == 0 else d_raw[side, columns]
                new.append(work[side, columns] * inv_alpha - keep * old)
                d_raw[side, columns] = new[-1]
            keep_data(real, imag, columns, *[x.astype(BF16) for x in new])
            return fold(new[0] * new[0] + new[1] * new[1])

        return body

    @pl.loop(0, m - 1 if shadow else m)
    def _(s):
        for h in range(parts):
            @pl.when(s > 0)
            def _():
                for p in range(2):
                    @pl.when(z - s >= 0)
                    def _():
                        await_piece(z - s, c, h, p)
                        spread(z - s, h, p, True, False)

                    @pl.when(z + s < m)
                    def _():
                        await_piece(z + s, c, h, p)
                        spread(z + s, h, p, False, True)

            @pl.loop(0, 2)
            def _(up):
                zb = z - s + 2 * s * up

                @pl.when((zb >= 0) & (zb < m) & ((s > 0) | (up == 0)))
                def _():
                    for p in range(2):
                        await_piece(zb, 1 - c, h, p)
                    if overlap:
                        process(zb * parts + h)

    if not overlap:
        @pl.loop(0, order // unit)
        def _(u):
            process(u)

    def first_update():
        return update_data(0, jnp.sqrt(finish_cast(0, voters)[0]), beta)

    if shadow:
        @pl.when(jnp.logical_not(edge))
        def _():
            @pl.when((z == 1) | (z == m - 2))
            def _():
                home = jnp.where(z == 1, 0, m - 1)
                if parts == 1:
                    mine = [(home * 2 + c) * rows]
                    high = rows
                else:
                    mine = [(home * parts + c) * unit]
                    high = unit
                mine = [pl.ds(pl.multiple_of(x, high), high) for x in mine]
                for low in mine:
                    @pl.loop(0, order // unit)
                    def _(u):
                        band = pl.ds(pl.multiple_of(u * unit, unit), unit)
                        slices = band_columns(u)
                        for p in range(2):
                            fit = dot_t(full[p, low, :], full[0, band, :])
                            other = dot_t(full[1 - p, low, :], full[1, band, :])
                            fit = fit - other if p else fit + other
                            x = jnp.concatenate([full[p, low, s] for s in slices], axis=1)
                            raw = (x.astype(F32) - weight * fit) * inv_first
                            stats[1, 0] += fold(raw * raw)

            start_cast(0)
            sweep(first_update(), 2)

        @pl.when(edge)
        def _():
            zb = m - 1 - z
            for h in range(parts):
                u = zb * parts + h
                for p in range(2):
                    await_piece(zb, c, h, p)
                    block_copy(2, zb, c, h, p, sibling).start()
                    await_piece(zb, 1 - c, h, p)
                    if p == 0 and h == parts - 1:
                        begin(u)
                if h < parts - 1:
                    process(u)
                else:
                    process(u, True, first_update())
    else:
        start_cast(0)
        sweep(first_update(), 2)

    alpha = jnp.sqrt(read_cast(0, voters)[0])
    phi_bar, rho_bar = beta, alpha
    direction, answer = [1.0 / alpha], []
    everyone = range(n)
    for it in range(ITERS):
        last = it == ITERS - 1
        ka, kb = 2 * it, 2 * it + 1
        model_ref = models[it]

        def forward_block(i):
            fit = forward_fit(pl.ds(0, order), block(i))
            work[:, block(i)] = model_ref[:, block(i)] - weight * fit

        def adjoint_block(i):
            image[:, block(i)] = d_raw[:, block(i)] - weight * regroup(adjoint_fit(block(i)))

        if it > 0:
            for i in range(count - 1):
                forward_block(i)
            alpha = jnp.sqrt(finish_cast(ka, everyone)[0])
            rotate(alpha)
            body = update_data(it, alpha, beta)
            tiles(body, kb + 1, range(count - 1))
            forward_block(count - 1)
            tiles(body, kb + 1, range(count - 1, count))
        start_cast(kb)

        if last:
            def products(real, imag, columns):
                xr, xi = image[real, columns], image[imag, columns]
                stats[kb + 2, 1] += fold(xr * model_ref[real, columns] + xi * model_ref[imag, columns])
                return fold(xr * xr + xi * xi)

            for i in range(count):
                adjoint_block(i)
                tiles(products, kb + 2, range(i - 1, i) if i else ())
            tiles(products, kb + 2, range(count - 1, count))
            start_cast(kb + 1)
        else:
            for i in range(count - 1):
                adjoint_block(i)

        data_sq = finish_cast(kb, everyone)[0]
        beta = jnp.sqrt(data_sq)
        inv_beta, shift = 1.0 / beta, beta / alpha

        if not last:
            def update_model(real, imag, columns):
                new = []
                for side in (real, imag):
                    new.append(image[side, columns] * inv_beta - shift * model_ref[side, columns])
                    models[it + 1][side, columns] = new[-1]
                keep_model(real, imag, columns, *[regroup(x.astype(BF16)) for x in new])
                return fold(new[0] * new[0] + new[1] * new[1])

            tiles(update_model, kb + 2, range(count - 1))
            adjoint_block(count - 1)
            tiles(update_model, kb + 2, range(count - 1, count))
            start_cast(kb + 1)

        rho = jnp.sqrt(rho_bar * rho_bar + beta * beta)
        cosine, sine = rho_bar / rho, beta / rho
        step = cosine * phi_bar / rho
        phi_bar = sine * phi_bar
        answer = [x + step * w for x, w in zip(answer + [0.0], direction)]

        def rotate(alpha, sine=sine, cosine=cosine, rho=rho):
            nonlocal rho_bar, direction
            rho_bar = -cosine * alpha
            turn = sine * alpha / rho
            direction = [-turn * w for w in direction] + [1.0 / alpha]

    def combine_basis(real, imag, columns):
        for side in (real, imag):
            basis = [model[side, columns] for model in models]
            fresh = image[side, columns]
            models[0][side, columns] = sum(w * x for w, x in zip(answer[1:], basis[1:])) + answer[0] * basis[0]
            models[1][side, columns] = sum(w * x for w, x in zip(direction[1:], basis[1:])) + direction[0] * basis[0]
            image[side, columns] = inv_beta * fresh - shift * basis[-1]

    sweep(combine_basis, None)
    drain_sum()
    pl.when(votes)(lambda: drain_cast(0))
    for k in range(1, 2 * ITERS):
        drain_cast(k)

    settle()

    image_sq, cross = finish_cast(2 * ITERS, everyone)
    new_alpha = jnp.sqrt(image_sq / data_sq - 2.0 * cross / alpha + data_sq)
    coef[0:1, :] = jnp.broadcast_to(-sine * new_alpha / rho, (1, 128))
    coef[1:2, :] = jnp.broadcast_to(1.0 / new_alpha, (1, 128))
    drain_cast(2 * ITERS)


def combine(coef, ready, turned, fresh, answer, direction, staged, sem):
    rows, order = answer.shape[2], answer.shape[3]
    high = min(rows, 64)
    per = rows // high

    def leave(o, p, i):
        source, out = ((ready, answer), (staged, direction))[o]
        return pltpu.make_async_copy(
            source.at[pl.ds(p * rows + i * high, high), :],
            out.at[0, p, pl.ds(i * high, high), :],
            sem.at[o, p, i],
        )

    tiles = [(p, i) for p in range(2) for i in range(per)]
    for p, i in tiles:
        leave(0, p, i).start()
    old, new = coef[0:1, 0:1], coef[1:2, 0:1]
    for p, i in tiles:
        band = pl.ds(p * rows + i * high, high)
        staged[band, :] = old * turned[band, :] + new * fresh[band, :]
        leave(1, p, i).start()
    for p, i in tiles:
        for o in range(2):
            leave(o, p, i).wait()


def on_device(n, nf, data):
    rows, order = data.shape[2], data.shape[3]
    weight = 1.0 / (3.0 * (2.0 * order) ** 0.5)
    wide, parts = block_sizes(rows, order)
    unit = 2 * rows // parts if rows % 128 == 0 else min(order, 256)
    field = pltpu.VMEM((2 * rows, order), F32)
    rounded = pltpu.VMEM((2 * rows, order), BF16)
    tile = pltpu.VMEM((8, 128), F32)
    casts = 1 + 2 * ITERS
    dma = pltpu.SemaphoreType.DMA
    vmem = pl.BlockSpec(memory_space=pltpu.VMEM)
    anywhere = pl.BlockSpec(memory_space=pl.ANY)
    *basis, coef = pl.pallas_call(
        functools.partial(kernel, n, nf, weight),
        out_shape=(field,) * (ITERS + 1) + (tile,),
        in_specs=[anywhere],
        out_specs=(vmem,) * (ITERS + 2),
        scratch_shapes=[
            pltpu.VMEM((2, order, order), BF16),
            rounded, rounded, rounded, rounded, field, field,
            pltpu.VMEM((2 * rows, unit), F32),
            pltpu.VMEM((casts + 1, 2, 8, 128), F32),
            pltpu.VMEM((n, 8, 128), F32), tile, pltpu.VMEM((nf, 8, 128), F32),
            pltpu.VMEM((casts, 1, 128), F32), pltpu.VMEM((casts, n * nf, 1, 128), F32),
            dma((2 * parts + 2,)), dma((3,)), dma((n, parts, 2)),
            dma((4,)), dma((casts,)), dma((casts,)),
        ],
        compiler_params=pltpu.CompilerParams(
            collective_id=0, has_side_effects=True, vmem_limit_bytes=46 * 2**20
        ),
    )(data)
    out = jax.ShapeDtypeStruct(data.shape, F32)
    high = min(rows, 64)
    return pl.pallas_call(
        combine,
        out_shape=(out, out),
        in_specs=[vmem] * (ITERS + 2),
        out_specs=(anywhere, anywhere),
        scratch_shapes=[pltpu.VMEM((2 * rows, order), F32), dma((2, 2, rows // high))],
        compiler_params=pltpu.CompilerParams(vmem_limit_bytes=24 * 2**20),
    )(coef, *basis)


def solution(mesh):
    spec = P("freq", None, "row", None)
    return jax.shard_map(
        functools.partial(on_device, mesh.shape["row"], mesh.shape["freq"]),
        mesh=mesh,
        in_specs=(spec,),
        out_specs=(spec, spec),
        check_vma=False,
    )
```
